128 devices in a mesh: dp: 8 (over y_lo, x), tensor: 16 (over y_hi, z, core).
Axes of the slice: x: 4, y: 4 (y_hi: 2, y_lo: 2; y = y_hi * 2 + y_lo), z: 4, core: 2. Of those that a mesh axis runs over, the one named last changes fastest.
Arguments:
- saved_input: bfloat16 [1024, 8192], P(('dp', 'tensor')), may hold values from -8 to 8
- keep_bits: int32 [1024, 448], P(('dp', 'tensor')), may hold values from -2147483648 to 2147483646, as said below
- norm_gain: bfloat16 [8192], P('dp'), may hold values from 0.099609375 to 1.8984375
- gate_weight: bfloat16 [8192, 14336], P('dp', 'tensor'), may hold values from -0.0625 to 0.0625
- up_weight: bfloat16 [8192, 14336], P('dp', 'tensor'), may hold values from -0.0625 to 0.0625
- down_weight: bfloat16 [14336, 8192], P('tensor', 'dp'), may hold values from -0.046875 to 0.046875
Outputs:
- layer_out: bfloat16 [1024, 8192], P('tensor', 'dp')
- row_check: float32 [1024], P('tensor')
The draws below stay inside these ranges and needn't reach their ends.
Inputs may be any that keep to these rules, and one draw needn't show every extreme that they name: `keep_bits`: bit k of word w of a token is the keep bit of hidden unit 32 w + k.
All inputs are finite; a program needn't handle non-finite values.
Results may differ from the reference program's by a relative error of at most 0.017.
Values may be sent and summed in bfloat16 or wider, within the bound.
A program may use at most 64 MiB of HBM per device.

```python
import jax
import jax.numpy as jnp
from jax import lax

D = 8192
FF = 14336
TOKENS = 1024
WORDS = 448


def draw_saved_input(key, part):
    keys = jax.random.split(jax.random.fold_in(key, 11), 2)
    base = jax.random.normal(keys[0], (TOKENS, D), jnp.float32)
    rough = jnp.exp(jax.random.uniform(keys[1], (1, D), jnp.float32, -0.35, 0.35))
    rising = jnp.exp(jnp.linspace(-0.55, 0.55, D, dtype=jnp.float32))[None, :]
    values = base * rough * rising
    return jnp.clip(values, -8.0, 8.0).astype(jnp.bfloat16)


def draw_keep_bits(key, part):
    return jax.random.randint(jax.random.fold_in(key, 23), (TOKENS, WORDS), -2147483648, 2147483647, jnp.int32)


def block_levels(own_key, shape, shards, low, high):
    def one(dim, parts):
        heights = jax.random.uniform(jax.random.fold_in(jax.random.fold_in(own_key, 6), dim), (parts,), jnp.float32, low / len(shards), high / len(shards))
        return jnp.repeat(jnp.exp(heights), shape[dim] // parts).reshape((-1,) + (1,) * (len(shape) - dim - 1))

    gain = one(*shards[0])
    for cut in shards[1:]:
        gain = gain * one(*cut)
    return gain


def scatter_about(stream_key, dims, deviation, most, cuts=(), kind=jnp.bfloat16):
    level = block_levels(stream_key, dims, cuts, -0.22, 0.18) if cuts else 1.0
    result = jax.random.normal(stream_key, dims, jnp.float32) * deviation * level
    return jnp.minimum(jnp.maximum(result, -most), most).astype(kind)


def setup_inputs(seed: int = 0) -> dict:
    arg_keys = jax.random.split(jax.random.key(seed), 7)
    return {
        "saved_input": draw_saved_input(jax.random.fold_in(arg_keys[6], 71), 0),
        "keep_bits": draw_keep_bits(jax.random.fold_in(arg_keys[6], 71), 0),
        "norm_gain": jnp.clip(1.0 + 0.18 * jax.random.normal(arg_keys[2], (D,), jnp.float32), 0.099609375, 1.8984375).astype(jnp.bfloat16),
        "gate_weight": scatter_about(arg_keys[3], (D, FF), D ** -0.5, 0.0625, ((0, 8), (1, 16))),
        "up_weight": scatter_about(arg_keys[4], (D, FF), D ** -0.5, 0.0625, ((0, 8), (1, 16))),
        "down_weight": scatter_about(arg_keys[5], (FF, D), FF ** -0.5, 0.046875, ((0, 16), (1, 8))),
    }


def reference(saved_input, keep_bits, norm_gain, gate_weight, up_weight, down_weight):
    widened = saved_input.astype(jnp.float32)
    inv_rms = lax.rsqrt(lax.optimization_barrier(jnp.sum(widened * widened, axis=1, keepdims=True)) / D + 1e-05)
    normed = (widened * inv_rms * norm_gain.astype(jnp.float32)).astype(jnp.bfloat16)
    gate = jnp.dot(normed, gate_weight, preferred_element_type=jnp.float32)
    up_sum = jnp.dot(normed, up_weight, preferred_element_type=jnp.float32)
    shifts = jnp.arange(32, dtype=jnp.int32)
    keep_mask = jnp.bitwise_and(jnp.right_shift(keep_bits[:, :, None], shifts[None, None, :]), 1)
    keep_mask = keep_mask.reshape(keep_bits.shape[0], -1)
    hidden = (jax.nn.silu(gate) * up_sum * (2.0 * keep_mask.astype(jnp.float32))).astype(jnp.bfloat16)
    layer_out = (widened + jnp.dot(hidden, down_weight, preferred_element_type=jnp.float32)).astype(jnp.bfloat16)
    widened_out = layer_out.astype(jnp.float32)
    row_check = lax.optimization_barrier(jnp.sum(widened_out * widened_out, axis=1)) / D
    return (layer_out, row_check)
```

```python
import jax
import jax.numpy as jnp
from jax import lax
from jax.experimental import pallas as pl
from jax.experimental.pallas import tpu as pltpu
from jax.sharding import PartitionSpec as P

D = 8192
DS = 1024
FU = 896
MESH = pl.DeviceIdType.MESH
F32 = jnp.float32
BF16 = jnp.bfloat16
NX, NY, NH, NZ = 4, 2, 2, 4
OFFSETS = (0, 1, 3, 2)


def kernel(
    x_ref,
    kb_ref,
    gain_ref,
    wg_ref,
    wu_ref,
    wd_ref,
    out_ref,
    rc_ref,
    w,
    wd,
    spread,
    xb,
    xn,
    part,
    relay,
    rx,
    ysend,
    yrecv,
    hid,
    osum,
    orecv,
    fsend,
    frecv,
    csend,
    crecv,
    w_sem,
    l_sem,
    a_send,
    a_recv,
    x_send,
    x_recv,
    r_send,
    r_recv,
    h_send,
    h_recv,
    o_send,
    o_recv,
    f_send,
    f_recv,
    c_send,
    c_recv,
):
    dp = lax.axis_index("dp")
    tp = lax.axis_index("tensor")
    x, y = lax.rem(dp, NX), lax.div(dp, NX)
    c, z, h = lax.rem(tp, 2), lax.rem(lax.div(tp, 2), NZ), lax.div(tp, 2 * NZ)

    def dev_d(dx, dy):
        return {"dp": lax.rem(y + dy, NY) * NX + lax.rem(x + dx, NX), "tensor": tp}

    def t_of(hh, zz, cc):
        return (hh * NZ + zz) * 2 + cc

    def dev_t(dh, dz, dc=0):
        t = t_of(lax.rem(h + dh, NH), lax.rem(z + dz, NZ), lax.rem(c + dc, 2))
        return {"dp": dp, "tensor": t}

    x_next, x_prev, x_far = dev_d(1, 0), dev_d(NX - 1, 0), None
    y_other = dev_d(0, 1)
    sib = dev_t(0, 0, 1)
    h_other = dev_t(1, 0)
    z_next, z_prev = dev_t(0, 1), dev_t(0, NZ - 1)
    sent = []

    def send(src, dst, ssem, rsem, device):
        copy = pltpu.make_async_remote_copy(
            src_ref=src,
            dst_ref=dst,
            send_sem=ssem,
            recv_sem=rsem,
            device_id=device,
            device_id_type=MESH,
        )
        copy.start()
        sent.append(copy)

    def arrived(dst, ssem, rsem, device):
        pltpu.make_async_remote_copy(
            src_ref=dst,
            dst_ref=dst,
            send_sem=ssem,
            recv_sem=rsem,
            device_id=device,
            device_id_type=MESH,
        ).wait_recv()

    dp_others = [(dx, dy) for dx in (1, 3, 2, 0) for dy in (0, 1) if (dx, dy) != (0, 0)]
    tp_others = [(dh, dz) for dz in (2, 1, 3, 0) for dh in (1, 0) if (dh, dz) != (0, 0)]

    loads = [
        pltpu.make_async_copy(wg_ref, w.at[0], w_sem.at[0]),
        pltpu.make_async_copy(wu_ref, w.at[1], w_sem.at[1]),
        pltpu.make_async_copy(wd_ref, wd, w_sem.at[2]),
    ]
    for load in loads:
        load.start()
    mine = x * NY + y
    own = [
        pltpu.make_async_copy(
            x_ref.at[:, pl.ds(pl.multiple_of(dp * DS, DS), DS)], xb.at[tp, mine], l_sem.at[0]
        ),
        pltpu.make_async_copy(kb_ref, xb.at[tp, pl.ds(8, 2)], l_sem.at[1]),
    ]
    for copy in own:
        copy.start()

    barrier = pltpu.get_barrier_semaphore()
    for dx, dy in dp_others:
        pl.semaphore_signal(barrier, inc=1, device_id=dev_d(dx, dy), device_id_type=MESH)
    for dh, dz in tp_others:
        pl.semaphore_signal(barrier, inc=1, device_id=dev_t(dh, dz), device_id_type=MESH)
    pl.semaphore_signal(barrier, inc=1, device_id=sib, device_id_type=MESH)
    pl.semaphore_wait(barrier, len(dp_others) + len(tp_others) + 1)

    for i, (dx, dy) in enumerate(dp_others):
        there = lax.rem(y + dy, NY) * NX + lax.rem(x + dx, NX)
        send(
            x_ref.at[:, pl.ds(pl.multiple_of(there * DS, DS), DS)],
            xb.at[tp, mine],
            a_send.at[i],
            a_recv.at[mine],
            dev_d(dx, dy),
        )
    row = lax.broadcasted_iota(jnp.int32, (128, FU), 0)
    col = lax.broadcasted_iota(jnp.int32, (128, FU), 1)
    place = ((col & 31) >> 3) * 28 + (col >> 5)
    spread[...] = jnp.where(row == place, 1.0, 0.0).astype(BF16)
    for copy in own:
        copy.wait()
    for i, (dx, dy) in enumerate(dp_others):
        g = lax.rem(x + dx, NX) * NY + lax.rem(y + dy, NY)
        arrived(xb.at[tp, g], a_send.at[i], a_recv.at[g], dev_d(dx, dy))

    count = [0]

    def push(t, device):
        send(xb.at[t], xb.at[t], x_send.at[count[0]], x_recv.at[t], device)
        count[0] += 1

    def here(t):
        arrived(xb.at[t], x_send.at[0], x_recv.at[t], sib)

    z1, z3, z2 = lax.rem(z + 1, NZ), lax.rem(z + 3, NZ), lax.rem(z + 2, NZ)
    hh = 1 - h
    push(tp, h_other)
    push(tp, z_next)
    push(tp, z_prev)
    push(tp, sib)
    across = t_of(hh, z, c)
    here(across)
    push(across, z_next)
    push(across, z_prev)
    push(across, sib)

    def gather_near():
        a, b = t_of(h, z1, c), t_of(h, z3, c)
        e, f = t_of(hh, z1, c), t_of(hh, z3, c)
        here(a)
        push(a, z_prev)
        push(a, sib)
        here(b)
        push(b, sib)
        here(f)
        push(f, z_next)
        push(f, sib)
        here(e)
        push(e, sib)

    def gather_far():
        a, b = t_of(h, z2, c), t_of(hh, z2, c)
        here(a)
        push(a, sib)
        here(b)
        push(b, sib)

    xn1, xp1, xf = lax.rem(x + 1, NX), lax.rem(x + 3, NX), lax.rem(x + 2, NX)

    def matmul(k):
        zz = lax.rem(z + OFFSETS[k], NZ)
        here(t_of(0, zz, 1 - c))
        here(t_of(1, zz, 1 - c))
        blocks = [t_of(a, zz, b) for a in range(2) for b in range(2)]
        gain = gain_ref[...].astype(F32)
        for g in range(8):
            for i in range(4):
                v = xb[blocks[i], g].astype(F32) * gain
                xn[pl.ds(g * 32 + i * 8, 8), :] = v
        lhs = xn[...].astype(BF16)
        for half in range(2):
            if k == 0:
                loads[half].wait()
            acc = jnp.dot(lhs, w[half], preferred_element_type=F32).astype(BF16)
            for g in range(4):
                part[k, g, half] = acc[g * 64 : (g + 1) * 64]
            if half == 0:
                send(part.at[k, xf, 0], relay.at[k, 0], r_send.at[k, 0], r_recv.at[k, 0], x_next)
                send(part.at[k, xp1, 0], rx.at[k, 1, 0], r_send.at[k, 4], r_recv.at[k, 4], x_prev)
            else:
                send(part.at[k, xf, 1], relay.at[k, 1], r_send.at[k, 1], r_recv.at[k, 1], x_prev)
                send(part.at[k, xn1, 1], rx.at[k, 0, 1], r_send.at[k, 3], r_recv.at[k, 3], x_next)

    def relay_sums(k):
        arrived(relay.at[k, 0], r_send.at[k, 0], r_recv.at[k, 0], x_next)
        v = part[k, xn1, 0].astype(F32) + relay[k, 0].astype(F32)
        part[k, xn1, 0] = v.astype(BF16)
        send(part.at[k, xn1, 0], rx.at[k, 0, 0], r_send.at[k, 2], r_recv.at[k, 2], x_next)
        arrived(relay.at[k, 1], r_send.at[k, 1], r_recv.at[k, 1], x_prev)
        v = part[k, xp1, 1].astype(F32) + relay[k, 1].astype(F32)
        part[k, xp1, 1] = v.astype(BF16)
        send(part.at[k, xp1, 1], rx.at[k, 1, 1], r_send.at[k, 5], r_recv.at[k, 5], x_prev)

    def x_sum(k, half, rows):
        return (
            part[k, x, half, rows, :].astype(F32)
            + rx[k, 0, half, rows, :].astype(F32)
            + rx[k, 1, half, rows, :].astype(F32)
        )

    def y_sums(k):
        arrived(rx.at[k, 1, 0], r_send.at[k, 4], r_recv.at[k, 4], x_prev)
        arrived(rx.at[k, 0, 1], r_send.at[k, 3], r_recv.at[k, 3], x_next)
        arrived(rx.at[k, 0, 0], r_send.at[k, 2], r_recv.at[k, 2], x_next)
        arrived(rx.at[k, 1, 1], r_send.at[k, 5], r_recv.at[k, 5], x_prev)
        rows = pl.ds(pl.multiple_of((1 - y) * 32, 32), 32)
        for half in range(2):
            ysend[k, half] = x_sum(k, half, rows).astype(BF16)
        send(ysend.at[k], yrecv.at[k], r_send.at[k, 6], r_recv.at[k, 6], y_other)

    def hidden(k):
        zz = lax.rem(z + OFFSETS[k], NZ)
        lanes = pl.ds(pl.multiple_of(lax.rem(tp, 8) * 128, 128), 128)
        slots = jnp.concatenate(
            [
                xb[t_of(a, zz, b), 8 + lax.div(tp, 8), :, lanes].astype(F32)
                for a in range(2)
                for b in range(2)
            ],
            axis=0,
        )
        lane = lax.broadcasted_iota(jnp.int32, (32, 128), 1)
        inv = jnp.sum(
            jnp.where((lane >= 112) & (lane < 115), slots, 0.0), axis=1, keepdims=True
        )
        byte = jnp.dot(slots.astype(BF16), spread[...], preferred_element_type=F32)
        unit = lax.broadcasted_iota(jnp.int32, (32, FU), 1)
        bit = (byte.astype(jnp.int32) >> (unit & 7)) & 1
        keep = 2.0 * bit.astype(F32)
        arrived(yrecv.at[k], r_send.at[k, 6], r_recv.at[k, 6], y_other)
        rows = pl.ds(pl.multiple_of(y * 32, 32), 32)
        gate = (x_sum(k, 0, rows) + yrecv[k, 0].astype(F32)) * inv
        up = (x_sum(k, 1, rows) + yrecv[k, 1].astype(F32)) * inv
        hid[k, x, y] = (gate / (1.0 + jnp.exp(-gate)) * up * keep).astype(BF16)
        for i, device in enumerate((x_next, x_prev, y_other)):
            send(hid.at[k, x, y], hid.at[k, x, y], h_send.at[k, i], h_recv.at[k, mine], device)

    def h_here(k, xx, yy):
        arrived(hid.at[k, xx, yy], h_send.at[k, 0], h_recv.at[k, xx * NY + yy], x_next)

    def pass_y(k):
        h_here(k, x, 1 - y)
        for i, device in enumerate((x_next, x_prev)):
            send(
                hid.at[k, x, 1 - y],
                hid.at[k, x, 1 - y],
                h_send.at[k, 3 + i],
                h_recv.at[k, x * NY + 1 - y],
                device,
            )

    def pass_x(k):
        h_here(k, xp1, 0)
        send(
            hid.at[k, xp1, 0], hid.at[k, xp1, 0], h_send.at[k, 5], h_recv.at[k, xp1 * NY], x_next
        )
        h_here(k, xn1, 1)
        send(
            hid.at[k, xn1, 1],
            hid.at[k, xn1, 1],
            h_send.at[k, 6],
            h_recv.at[k, xn1 * NY + 1],
            x_prev,
        )

    def down(k):
        h_here(k, xp1, 1)
        h_here(k, xn1, 0)
        h_here(k, xf, 0)
        h_here(k, xf, 1)
        if k == 0:
            loads[2].wait()
        lhs = hid[k].reshape(256, FU)
        acc = jnp.dot(lhs, wd[...], preferred_element_type=F32).astype(BF16)
        for g in range(8):
            for s in range(2):
                osum[k, s, g] = acc[g * 32 + s * 16 : g * 32 + s * 16 + 16]
        send(osum.at[k, 1 - c], orecv.at[k], o_send.at[k], o_recv.at[k], sib)

    def to_owners(k):
        zz = lax.rem(z + OFFSETS[k], NZ)
        arrived(orecv.at[k], o_send.at[k], o_recv.at[k], sib)
        fsend[k] = (osum[k, c].astype(F32) + orecv[k].astype(F32)).astype(BF16)
        here_index = h * NZ + z
        for i, (dh, dz) in enumerate(tp_others):
            g = lax.rem(z + dz, NZ) * NY + lax.rem(h + dh, NH)
            send(
                fsend.at[k, g],
                frecv.at[here_index, zz],
                f_send.at[k, i],
                f_recv.at[here_index, zz],
                dev_t(dh, dz),
            )

    matmul(0)
    gather_near()
    matmul(1)
    relay_sums(0)
    matmul(2)
    gather_far()
    relay_sums(1)
    y_sums(0)
    matmul(3)
    relay_sums(2)
    y_sums(1)
    hidden(0)
    relay_sums(3)
    y_sums(2)
    hidden(1)
    pass_y(0)
    y_sums(3)
    hidden(2)
    pass_y(1)
    pass_x(0)
    hidden(3)
    pass_y(2)
    pass_x(1)
    down(0)
    pass_y(3)
    pass_x(2)
    down(1)
    to_owners(0)
    pass_x(3)
    down(2)
    to_owners(1)
    down(3)
    to_owners(2)
    to_owners(3)

    squares = []
    for k in range(4):
        zz = lax.rem(z + OFFSETS[k], NZ)
        total = fsend[k, z * NY + h].astype(F32)
        res = jnp.concatenate(
            [xb[t_of(c, zz, b), z * NY + h].astype(F32) for b in range(2)], axis=0
        )
        total = total + res
        for i, (dh, dz) in enumerate(tp_others):
            src = lax.rem(h + dh, NH) * NZ + lax.rem(z + dz, NZ)
            arrived(frecv.at[src, zz], f_send.at[0, i], f_recv.at[src, zz], dev_t(dh, dz))
            total = total + frecv[src, zz].astype(F32)
        rounded = total.astype(BF16)
        out_ref[pl.ds(pl.multiple_of(zz * 16, 16), 16), :] = rounded
    wide = out_ref[...].astype(F32)
    wide = wide * wide
    folded = wide[:, 0:128]
    for i in range(1, 8):
        folded = folded + wide[:, i * 128 : (i + 1) * 128]
    rowsum = jnp.sum(folded.T, axis=0, keepdims=True)
    csend[:, 0:64] = jnp.broadcast_to(rowsum, (8, 64))
    csend[:, 64:128] = jnp.zeros((8, 64), F32)
    for i, (dx, dy) in enumerate(dp_others):
        send(csend, crecv.at[mine], c_send.at[i], c_recv.at[mine], dev_d(dx, dy))
    total = csend[...]
    for i, (dx, dy) in enumerate(dp_others):
        g = lax.rem(x + dx, NX) * NY + lax.rem(y + dy, NY)
        arrived(crecv.at[g], c_send.at[i], c_recv.at[g], dev_d(dx, dy))
        total = total + crecv[g]
    rc_ref[...] = total / D
    for copy in sent:
        copy.wait_send()


def on_device(saved_input, keep_bits, norm_gain, gate_weight, up_weight, down_weight):
    rows = saved_input.shape[0]
    wide = saved_input.astype(F32)
    inv = lax.rsqrt(jnp.sum(wide * wide, axis=1) / D + 1e-05)
    hi = lax.reduce_precision(inv, 8, 7)
    mid = lax.reduce_precision(inv - hi, 8, 7)
    low = lax.reduce_precision(inv - hi - mid, 8, 7)
    words = keep_bits.reshape(rows, 16, 28)
    parts = [((words >> (8 * j)) & 255).astype(F32) for j in range(4)]
    scale = jnp.stack((hi, mid, low), axis=1)[:, None, :]
    parts.append(jnp.broadcast_to(scale, (rows, 16, 3)))
    parts.append(jnp.zeros((rows, 16, 13), F32))
    slots = jnp.concatenate(parts, axis=2).reshape(rows, 2, 1024).transpose(1, 0, 2)
    slots = slots.astype(BF16)
    vmem = pl.BlockSpec(memory_space=pltpu.VMEM)
    hbm = pl.BlockSpec(memory_space=pl.ANY)
    dma = pltpu.SemaphoreType.DMA
    out, check = pl.pallas_call(
        kernel,
        out_shape=(
            jax.ShapeDtypeStruct((64, DS), BF16),
            jax.ShapeDtypeStruct((8, 128), F32),
        ),
        in_specs=[vmem, vmem, vmem, hbm, hbm, hbm],
        out_specs=(vmem, vmem),
        scratch_shapes=[
            pltpu.VMEM((2, DS, FU), BF16),
            pltpu.VMEM((FU, DS), BF16),
            pltpu.VMEM((128, FU), BF16),
            pltpu.VMEM((16, 10, 8, DS), BF16),
            pltpu.VMEM((256, DS), F32),
            pltpu.VMEM((4, 4, 2, 64, FU), BF16),
            pltpu.VMEM((4, 2, 64, FU), BF16),
            pltpu.VMEM((4, 2, 2, 64, FU), BF16),
            pltpu.VMEM((4, 2, 32, FU), BF16),
            pltpu.VMEM((4, 2, 32, FU), BF16),
            pltpu.VMEM((4, 4, 2, 32, FU), BF16),
            pltpu.VMEM((4, 2, 8, 16, DS), BF16),
            pltpu.VMEM((4, 8, 16, DS), BF16),
            pltpu.VMEM((4, 8, 16, DS), BF16),
            pltpu.VMEM((8, 4, 16, DS), BF16),
            pltpu.VMEM((8, 128), F32),
            pltpu.VMEM((8, 8, 128), F32),
            dma((3,)),
            dma((2,)),
            dma((7,)),
            dma((8,)),
            dma((15,)),
            dma((16,)),
            dma((4, 7)),
            dma((4, 7)),
            dma((4, 7)),
            dma((4, 8)),
            dma((4,)),
            dma((4,)),
            dma((4, 7)),
            dma((8, 4)),
            dma((7,)),
            dma((8,)),
        ],
        compiler_params=pltpu.CompilerParams(
            collective_id=0, has_side_effects=True, vmem_limit_bytes=56 * 1024 * 1024
        ),
        name="block",
    )(saved_input, slots, norm_gain.reshape(1, DS), gate_weight, up_weight, down_weight)
    return out, check[0, :64]


def solution(mesh):
    both = ("dp", "tensor")
    return jax.shard_map(
        on_device,
        mesh=mesh,
        in_specs=(
            P(both, None),
            P(both, None),
            P("dp"),
            P("dp", "tensor"),
            P("dp", "tensor"),
            P("tensor", "dp"),
        ),
        out_specs=(P("tensor", "dp"), P("tensor")),
        check_vma=False,
    )
```

```python
import jax
import jax.numpy as jnp
from jax import lax
from jax.experimental import pallas as pl
from jax.experimental.pallas import tpu as pltpu
from jax.sharding import PartitionSpec as P

D = 8192
DS = 1024
FU = 896
MESH = pl.DeviceIdType.MESH
F32 = jnp.float32
BF16 = jnp.bfloat16
NX, NY, NH, NZ = 4, 2, 2, 4
OFFSETS = (0, 1, 3, 2)


def kernel(
    x_ref,
    kb_ref,
    gain_ref,
    wg_hbm,
    wu_hbm,
    wd_hbm,
    out_ref,
    rc_ref,
    wg,
    wu,
    wd,
    spread,
    words,
    xb,
    xn,
    pg,
    pu,
    g_relay,
    g_recv,
    u_relay,
    u_recv,
    u_y,
    ysend,
    yrecv,
    hid,
    osum,
    orecv,
    fsend,
    frecv,
    csend,
    crecv,
    w_sem,
    l_sem,
    a_send,
    a_recv,
    x_send,
    x_recv,
    g_send,
    g_done,
    u_send,
    u_done,
    h_send,
    h_recv,
    o_send,
    o_recv,
    f_send,
    f_recv,
    c_send,
    c_recv,
):
    dp = lax.axis_index("dp")
    tp = lax.axis_index("tensor")
    x, y = lax.rem(dp, NX), lax.div(dp, NX)
    c, z, h = lax.rem(tp, 2), lax.rem(lax.div(tp, 2), NZ), lax.div(tp, 2 * NZ)

    def dev_d(dx, dy):
        return {"dp": lax.rem(y + dy, NY) * NX + lax.rem(x + dx, NX), "tensor": tp}

    def t_of(hh, zz, cc):
        return (hh * NZ + zz) * 2 + cc

    def dev_t(dh, dz, dc=0):
        t = t_of(lax.rem(h + dh, NH), lax.rem(z + dz, NZ), lax.rem(c + dc, 2))
        return {"dp": dp, "tensor": t}

    x_next, x_prev = dev_d(1, 0), dev_d(NX - 1, 0)
    y_other = dev_d(0, 1)
    sib = dev_t(0, 0, 1)
    h_other = dev_t(1, 0)
    z_next, z_prev = dev_t(0, 1), dev_t(0, NZ - 1)
    sent = []

    def send(src, dst, ssem, rsem, device):
        copy = pltpu.make_async_remote_copy(
            src_ref=src,
            dst_ref=dst,
            send_sem=ssem,
            recv_sem=rsem,
            device_id=device,
            device_id_type=MESH,
        )
        copy.start()
        sent.append(copy)

    def arrived(dst, ssem, rsem, device):
        pltpu.make_async_remote_copy(
            src_ref=dst,
            dst_ref=dst,
            send_sem=ssem,
            recv_sem=rsem,
            device_id=device,
            device_id_type=MESH,
        ).wait_recv()

    dp_others = [(dx, dy) for dx in (1, 3, 2, 0) for dy in (0, 1) if (dx, dy) != (0, 0)]
    tp_others = [(dh, dz) for dz in (2, 1, 3, 0) for dh in (1, 0) if (dh, dz) != (0, 0)]

    loads = [
        pltpu.make_async_copy(wu_hbm, wu, w_sem.at[0]),
        pltpu.make_async_copy(wg_hbm, wg, w_sem.at[1]),
        pltpu.make_async_copy(wd_hbm, wd, w_sem.at[2]),
    ]
    for load in loads:
        load.start()
    mine = x * NY + y
    own = pltpu.make_async_copy(
        x_ref.at[:, pl.ds(pl.multiple_of(dp * DS, DS), DS)], xb.at[tp, mine], l_sem
    )
    own.start()

    barrier = pltpu.get_barrier_semaphore()
    for dx, dy in dp_others:
        pl.semaphore_signal(barrier, inc=1, device_id=dev_d(dx, dy), device_id_type=MESH)
    for dh, dz in tp_others:
        pl.semaphore_signal(barrier, inc=1, device_id=dev_t(dh, dz), device_id_type=MESH)
    pl.semaphore_signal(barrier, inc=1, device_id=sib, device_id_type=MESH)
    wide = x_ref[...].astype(F32)
    inv = lax.rsqrt(jnp.sum(wide * wide, axis=1, keepdims=True) / D + 1e-05)
    hi = inv.astype(BF16).astype(F32)
    mid = (inv - hi).astype(BF16).astype(F32)
    low = inv - hi - mid
    words[...] = jnp.zeros((8, 512), jnp.int32)
    words[:, 0:448] = kb_ref[...]
    lane = lax.broadcasted_iota(jnp.int32, (8, 128), 1)
    scale = jnp.where(lane == 112, hi, jnp.where(lane == 113, mid, low))
    scale = jnp.where((lane >= 112) & (lane < 115), scale, 0.0)
    for t in range(16):
        tile, start = divmod(28 * t, 128)
        piece = words[:, tile * 128 : tile * 128 + 128]
        if start:
            piece = pltpu.roll(piece, 128 - start, 1)
        if start + 28 > 128:
            after = pltpu.roll(words[:, tile * 128 + 128 : tile * 128 + 256], 128 - start, 1)
            piece = jnp.where(lane < 128 - start, piece, after)
        taken = jnp.zeros((8, 128), jnp.int32)
        for j in range(4):
            byte = (piece >> (8 * j)) & 255
            if j:
                byte = pltpu.roll(byte, 28 * j, 1)
            taken = jnp.where((lane >= 28 * j) & (lane < 28 * j + 28), byte, taken)
        slot = (taken.astype(F32) + scale).astype(BF16)
        xb[tp, 8 + t // 8, :, (t % 8) * 128 : (t % 8) * 128 + 128] = slot
    pl.semaphore_wait(barrier, len(dp_others) + len(tp_others) + 1)

    for i, (dx, dy) in enumerate(dp_others):
        there = lax.rem(y + dy, NY) * NX + lax.rem(x + dx, NX)
        send(
            x_ref.at[:, pl.ds(pl.multiple_of(there * DS, DS), DS)],
            xb.at[tp, mine],
            a_send.at[i],
            a_recv.at[mine],
            dev_d(dx, dy),
        )
    row = lax.broadcasted_iota(jnp.int32, (128, FU), 0)
    col = lax.broadcasted_iota(jnp.int32, (128, FU), 1)
    place = ((col & 31) >> 3) * 28 + (col >> 5)
    spread[...] = jnp.where(row == place, 1.0, 0.0).astype(BF16)
    own.wait()
    for i, (dx, dy) in enumerate(dp_others):
        g = lax.rem(x + dx, NX) * NY + lax.rem(y + dy, NY)
        arrived(xb.at[tp, g], a_send.at[i], a_recv.at[g], dev_d(dx, dy))

    count = [0]

    def push(t, device):
        send(xb.at[t], xb.at[t], x_send.at[count[0]], x_recv.at[t], device)
        count[0] += 1

    def here(t):
        arrived(xb.at[t], x_send.at[0], x_recv.at[t], sib)

    z1, z3, z2 = lax.rem(z + 1, NZ), lax.rem(z + 3, NZ), lax.rem(z + 2, NZ)
    hh = 1 - h
    push(tp, h_other)
    push(tp, z_next)
    push(tp, z_prev)
    push(tp, sib)
    across = t_of(hh, z, c)
    here(across)
    push(across, z_next)
    push(across, z_prev)
    push(across, sib)

    def gather_near():
        a, b = t_of(h, z1, c), t_of(h, z3, c)
        e, f = t_of(hh, z1, c), t_of(hh, z3, c)
        here(a)
        push(a, z_prev)
        push(a, sib)
        here(b)
        push(b, sib)
        here(f)
        push(f, z_next)
        push(f, sib)
        here(e)
        push(e, sib)

    def gather_far():
        a, b = t_of(h, z2, c), t_of(hh, z2, c)
        here(a)
        push(a, sib)
        here(b)
        push(b, sib)

    xn1, xp1, xf = lax.rem(x + 1, NX), lax.rem(x + 3, NX), lax.rem(x + 2, NX)

    def matmul(k):
        zz = lax.rem(z + OFFSETS[k], NZ)
        here(t_of(0, zz, 1 - c))
        here(t_of(1, zz, 1 - c))
        blocks = [t_of(a, zz, b) for a in range(2) for b in range(2)]
        gain = gain_ref[...].astype(F32).reshape(1, DS)
        for g in range(8):
            for i in range(4):
                v = xb[blocks[i], g].astype(F32) * gain
                xn[pl.ds(g * 32 + i * 8, 8), :] = v
        lhs = xn[...].astype(BF16)
        if k == 0:
            loads[0].wait()
        acc = jnp.dot(lhs, wu[...], preferred_element_type=F32).astype(BF16)
        for g in range(8):
            for i in range(2):
                lo = g * 32 + i * 16
                pu[k, g % 2, g // 2, i] = acc[lo : lo + 16]
        send(pu.at[k, 1 - y], u_y.at[k], u_send.at[k, 0], u_done.at[k, 0], y_other)
        if k == 0:
            loads[1].wait()
        acc = jnp.dot(lhs, wg[...], preferred_element_type=F32).astype(BF16)
        for g in range(8):
            pg[k, g // 2, g % 2] = acc[g * 32 : g * 32 + 32]
        send(pg.at[k, xf, 0], g_relay.at[k, 0], g_send.at[k, 0], g_done.at[k, 0], x_next)
        send(pg.at[k, xf, 1], g_relay.at[k, 1], g_send.at[k, 1], g_done.at[k, 1], x_prev)
        send(pg.at[k, xn1, 1], g_recv.at[k, 0, 1], g_send.at[k, 3], g_done.at[k, 3], x_next)
        send(pg.at[k, xp1, 0], g_recv.at[k, 1, 0], g_send.at[k, 4], g_done.at[k, 4], x_prev)

    def gate_relay(k):
        arrived(g_relay.at[k, 0], g_send.at[k, 0], g_done.at[k, 0], x_next)
        v = pg[k, xn1, 0].astype(F32) + g_relay[k, 0].astype(F32)
        pg[k, xn1, 0] = v.astype(BF16)
        send(pg.at[k, xn1, 0], g_recv.at[k, 0, 0], g_send.at[k, 2], g_done.at[k, 2], x_next)
        arrived(g_relay.at[k, 1], g_send.at[k, 1], g_done.at[k, 1], x_prev)
        v = pg[k, xp1, 1].astype(F32) + g_relay[k, 1].astype(F32)
        pg[k, xp1, 1] = v.astype(BF16)
        send(pg.at[k, xp1, 1], g_recv.at[k, 1, 1], g_send.at[k, 5], g_done.at[k, 5], x_prev)

    def gate_over_x(k, yy):
        return (
            pg[k, x, yy].astype(F32) + g_recv[k, 0, yy].astype(F32) + g_recv[k, 1, yy].astype(F32)
        )

    def gate_y(k):
        arrived(g_recv.at[k, 0, 1], g_send.at[k, 3], g_done.at[k, 3], x_next)
        arrived(g_recv.at[k, 1, 0], g_send.at[k, 4], g_done.at[k, 4], x_prev)
        arrived(g_recv.at[k, 0, 0], g_send.at[k, 2], g_done.at[k, 2], x_next)
        arrived(g_recv.at[k, 1, 1], g_send.at[k, 5], g_done.at[k, 5], x_prev)
        ysend[k] = gate_over_x(k, 1 - y).astype(BF16)
        send(ysend.at[k], yrecv.at[k], g_send.at[k, 6], g_done.at[k, 6], y_other)

    def up_over_y(k):
        arrived(u_y.at[k], u_send.at[k, 0], u_done.at[k, 0], y_other)
        for xx in (xf, xn1, xp1, x):
            v = pu[k, y, xx].astype(F32) + u_y[k, xx].astype(F32)
            pu[k, y, xx] = v.astype(BF16)
            if xx is xf:
                send(pu.at[k, y, xf, 0], u_relay.at[k, 0], u_send.at[k, 1], u_done.at[k, 1], x_next)
                send(pu.at[k, y, xf, 1], u_relay.at[k, 1], u_send.at[k, 2], u_done.at[k, 2], x_prev)
            if xx is xn1:
                send(
                    pu.at[k, y, xx, 1], u_recv.at[k, 0, 1], u_send.at[k, 3], u_done.at[k, 3], x_next
                )
            if xx is xp1:
                send(
                    pu.at[k, y, xx, 0], u_recv.at[k, 1, 0], u_send.at[k, 4], u_done.at[k, 4], x_prev
                )

    def up_relay(k):
        arrived(u_relay.at[k, 0], u_send.at[k, 1], u_done.at[k, 1], x_next)
        v = pu[k, y, xn1, 0].astype(F32) + u_relay[k, 0].astype(F32)
        pu[k, y, xn1, 0] = v.astype(BF16)
        send(pu.at[k, y, xn1, 0], u_recv.at[k, 0, 0], u_send.at[k, 5], u_done.at[k, 5], x_next)
        arrived(u_relay.at[k, 1], u_send.at[k, 2], u_done.at[k, 2], x_prev)
        v = pu[k, y, xp1, 1].astype(F32) + u_relay[k, 1].astype(F32)
        pu[k, y, xp1, 1] = v.astype(BF16)
        send(pu.at[k, y, xp1, 1], u_recv.at[k, 1, 1], u_send.at[k, 6], u_done.at[k, 6], x_prev)

    def hidden(k):
        zz = lax.rem(z + OFFSETS[k], NZ)
        lanes = pl.ds(pl.multiple_of(lax.rem(tp, 8) * 128, 128), 128)
        slots = jnp.concatenate(
            [
                xb[t_of(a, zz, b), 8 + lax.div(tp, 8), :, lanes].astype(F32)
                for a in range(2)
                for b in range(2)
            ],
            axis=0,
        )
        lane = lax.broadcasted_iota(jnp.int32, (32, 128), 1)
        inv = jnp.sum(
            jnp.where((lane >= 112) & (lane < 115), slots, 0.0), axis=1, keepdims=True
        )
        byte = jnp.dot(slots.astype(BF16), spread[...], preferred_element_type=F32)
        unit = lax.broadcasted_iota(jnp.int32, (32, FU), 1)
        bit = (byte.astype(jnp.int32) >> (unit & 7)) & 1
        keep = 2.0 * bit.astype(F32)
        arrived(yrecv.at[k], g_send.at[k, 6], g_done.at[k, 6], y_other)
        gate = (gate_over_x(k, y) + yrecv[k].astype(F32)) * inv
        arrived(u_recv.at[k, 0, 1], u_send.at[k, 3], u_done.at[k, 3], x_next)
        arrived(u_recv.at[k, 1, 0], u_send.at[k, 4], u_done.at[k, 4], x_prev)
        arrived(u_recv.at[k, 0, 0], u_send.at[k, 5], u_done.at[k, 5], x_next)
        arrived(u_recv.at[k, 1, 1], u_send.at[k, 6], u_done.at[k, 6], x_prev)
        up = pu[k, y, x].astype(F32) + u_recv[k, 0].astype(F32) + u_recv[k, 1].astype(F32)
        up = up.reshape(32, FU) * inv
        hid[k, x, y] = (gate / (1.0 + jnp.exp(-gate)) * up * keep).astype(BF16)
        for i, device in enumerate((x_next, x_prev, y_other)):
            send(hid.at[k, x, y], hid.at[k, x, y], h_send.at[k, i], h_recv.at[k, mine], device)

    def h_here(k, xx, yy):
        arrived(hid.at[k, xx, yy], h_send.at[k, 0], h_recv.at[k, xx * NY + yy], x_next)

    def pass_y(k):
        h_here(k, x, 1 - y)
        for i, device in enumerate((x_next, x_prev)):
            send(
                hid.at[k, x, 1 - y],
                hid.at[k, x, 1 - y],
                h_send.at[k, 3 + i],
                h_recv.at[k, x * NY + 1 - y],
                device,
            )

    def pass_x(k):
        h_here(k, xp1, 0)
        send(
            hid.at[k, xp1, 0], hid.at[k, xp1, 0], h_send.at[k, 5], h_recv.at[k, xp1 * NY], x_next
        )
        h_here(k, xn1, 1)
        send(
            hid.at[k, xn1, 1],
            hid.at[k, xn1, 1],
            h_send.at[k, 6],
            h_recv.at[k, xn1 * NY + 1],
            x_prev,
        )

    def down(k):
        h_here(k, xp1, 1)
        h_here(k, xn1, 0)
        h_here(k, xf, 0)
        h_here(k, xf, 1)
        if k == 0:
            loads[2].wait()
        lhs = hid[k].reshape(256, FU)
        acc = jnp.dot(lhs, wd[...], preferred_element_type=F32).astype(BF16)
        for g in range(8):
            for s in range(2):
                osum[k, s, g] = acc[g * 32 + s * 16 : g * 32 + s * 16 + 16]
        send(osum.at[k, 1 - c], orecv.at[k], o_send.at[k], o_recv.at[k], sib)

    def to_owners(k):
        zz = lax.rem(z + OFFSETS[k], NZ)
        arrived(orecv.at[k], o_send.at[k], o_recv.at[k], sib)
        fsend[k] = (osum[k, c].astype(F32) + orecv[k].astype(F32)).astype(BF16)
        here_index = h * NZ + z
        for i, (dh, dz) in enumerate(tp_others):
            g = lax.rem(z + dz, NZ) * NY + lax.rem(h + dh, NH)
            send(
                fsend.at[k, g],
                frecv.at[here_index, zz],
                f_send.at[k, i],
                f_recv.at[here_index, zz],
                dev_t(dh, dz),
            )

    matmul(0)
    gather_near()
    gate_relay(0)
    matmul(2)
    matmul(1)
    gate_y(0)
    up_over_y(0)
    gather_far()
    matmul(3)
    up_over_y(2)
    gate_relay(3)
    up_relay(0)
    up_over_y(1)
    gate_relay(1)
    gate_relay(2)
    hidden(0)
    up_relay(1)
    up_relay(2)
    gate_y(1)
    gate_y(2)
    up_over_y(3)
    gate_y(3)
    pass_y(0)
    hidden(1)
    hidden(2)
    pass_x(0)
    pass_y(1)
    up_relay(3)
    pass_y(2)
    down(0)
    pass_x(1)
    hidden(3)
    pass_x(2)
    to_owners(0)
    down(1)
    pass_y(3)
    to_owners(1)
    down(2)
    pass_x(3)
    to_owners(2)
    down(3)
    to_owners(3)

    for k in range(4):
        zz = lax.rem(z + OFFSETS[k], NZ)
        total = fsend[k, z * NY + h].astype(F32)
        res = jnp.concatenate(
            [xb[t_of(c, zz, b), z * NY + h].astype(F32) for b in range(2)], axis=0
        )
        total = total + res
        for i, (dh, dz) in enumerate(tp_others):
            src = lax.rem(h + dh, NH) * NZ + lax.rem(z + dz, NZ)
            arrived(frecv.at[src, zz], f_send.at[0, i], f_recv.at[src, zz], dev_t(dh, dz))
            total = total + frecv[src, zz].astype(F32)
        rounded = total.astype(BF16)
        out_ref[pl.ds(pl.multiple_of(zz * 16, 16), 16), :] = rounded
    wide = out_ref[...].astype(F32)
    wide = wide * wide
    folded = wide[:, 0:128]
    for i in range(1, 8):
        folded = folded + wide[:, i * 128 : (i + 1) * 128]
    rowsum = jnp.sum(folded.T, axis=0, keepdims=True)
    csend[:, 0:64] = jnp.broadcast_to(rowsum, (8, 64))
    csend[:, 64:128] = jnp.zeros((8, 64), F32)
    for i, (dx, dy) in enumerate(dp_others):
        send(csend, crecv.at[mine], c_send.at[i], c_recv.at[mine], dev_d(dx, dy))
    total = csend[...]
    for i, (dx, dy) in enumerate(dp_others):
        g = lax.rem(x + dx, NX) * NY + lax.rem(y + dy, NY)
        arrived(crecv.at[g], c_send.at[i], c_recv.at[g], dev_d(dx, dy))
        total = total + crecv[g]
    rc_ref[...] = total[0, 0:64] / D
    for copy in sent:
        copy.wait_send()


def on_device(saved_input, keep_bits, norm_gain, gate_weight, up_weight, down_weight):
    vmem = pl.BlockSpec(memory_space=pltpu.VMEM)
    hbm = pl.BlockSpec(memory_space=pl.ANY)
    dma = pltpu.SemaphoreType.DMA
    out, check = pl.pallas_call(
        kernel,
        out_shape=(
            jax.ShapeDtypeStruct((64, DS), BF16),
            jax.ShapeDtypeStruct((64,), F32),
        ),
        in_specs=[vmem, vmem, vmem, hbm, hbm, hbm],
        out_specs=(vmem, vmem),
        scratch_shapes=[
            pltpu.VMEM((DS, FU), BF16),
            pltpu.VMEM((DS, FU), BF16),
            pltpu.VMEM((FU, DS), BF16),
            pltpu.VMEM((128, FU), BF16),
            pltpu.VMEM((8, 512), jnp.int32),
            pltpu.VMEM((16, 10, 8, DS), BF16),
            pltpu.VMEM((256, DS), F32),
            pltpu.VMEM((4, 4, 2, 32, FU), BF16),
            pltpu.VMEM((4, 2, 4, 2, 16, FU), BF16),
            pltpu.VMEM((4, 2, 32, FU), BF16),
            pltpu.VMEM((4, 2, 2, 32, FU), BF16),
            pltpu.VMEM((4, 2, 16, FU), BF16),
            pltpu.VMEM((4, 2, 2, 16, FU), BF16),
            pltpu.VMEM((4, 4, 2, 16, FU), BF16),
            pltpu.VMEM((4, 32, FU), BF16),
            pltpu.VMEM((4, 32, FU), BF16),
            pltpu.VMEM((4, 4, 2, 32, FU), BF16),
            pltpu.VMEM((4, 2, 8, 16, DS), BF16),
            pltpu.VMEM((4, 8, 16, DS), BF16),
            pltpu.VMEM((4, 8, 16, DS), BF16),
            pltpu.VMEM((8, 4, 16, DS), BF16),
            pltpu.VMEM((8, 128), F32),
            pltpu.VMEM((8, 8, 128), F32),
            dma((3,)),
            dma,
            dma((7,)),
            dma((8,)),
            dma((15,)),
            dma((16,)),
            dma((4, 7)),
            dma((4, 7)),
            dma((4, 7)),
            dma((4, 7)),
            dma((4, 7)),
            dma((4, 8)),
            dma((4,)),
            dma((4,)),
            dma((4, 7)),
            dma((8, 4)),
            dma((7,)),
            dma((8,)),
        ],
        compiler_params=pltpu.CompilerParams(
            collective_id=0, has_side_effects=True, vmem_limit_bytes=56 * 1024 * 1024
        ),
        name="block",
    )(saved_input, keep_bits, norm_gain, gate_weight, up_weight, down_weight)
    return out, check


def solution(mesh):
    both = ("dp", "tensor")
    return jax.shard_map(
        on_device,
        mesh=mesh,
        in_specs=(
            P(both, None),
            P(both, None),
            P("dp"),
            P("dp", "tensor"),
            P("dp", "tensor"),
            P("tensor", "dp"),
        ),
        out_specs=(P("tensor", "dp"), P("tensor")),
        check_vma=False,
    )
```

```python
import jax
import jax.numpy as jnp
from jax import lax
from jax.experimental import pallas as pl
from jax.experimental.pallas import tpu as pltpu
from jax.sharding import PartitionSpec as P

D = 8192
DS = 1024
FU = 896
MESH = pl.DeviceIdType.MESH
F32 = jnp.float32
BF16 = jnp.bfloat16
NX, NY, NH, NZ = 4, 2, 2, 4
OFFSETS = (0, 1, 3, 2)


def kernel(
    x_hbm,
    kb_ref,
    gain_ref,
    wg_hbm,
    wu_hbm,
    wd_hbm,
    out_ref,
    rc_ref,
    wg,
    wu,
    wd,
    spread,
    words,
    x_ref,
    xb,
    xn,
    pg,
    pu,
    g_relay,
    g_recv,
    u_relay,
    u_recv,
    u_y,
    ysend,
    yrecv,
    hid,
    osum,
    orecv,
    fsend,
    frecv,
    csend,
    crecv,
    w_sem,
    l_sem,
    a_send,
    a_recv,
    k_sem,
    x_send,
    x_recv,
    g_send,
    g_done,
    u_send,
    u_done,
    h_send,
    h_recv,
    o_send,
    o_recv,
    f_send,
    f_recv,
    c_send,
    c_recv,
):
    dp = lax.axis_index("dp")
    tp = lax.axis_index("tensor")
    x, y = lax.rem(dp, NX), lax.div(dp, NX)
    c, z, h = lax.rem(tp, 2), lax.rem(lax.div(tp, 2), NZ), lax.div(tp, 2 * NZ)

    def t_of(hh, zz, cc):
        return (hh * NZ + zz) * 2 + cc

    def dev_d(dx, dy, dh=0):
        d = lax.rem(y + dy, NY) * NX + lax.rem(x + dx, NX)
        return {"dp": d, "tensor": t_of(lax.rem(h + dh, NH), z, c)}

    def dev_t(dh, dz, dc=0):
        t = t_of(lax.rem(h + dh, NH), lax.rem(z + dz, NZ), lax.rem(c + dc, 2))
        return {"dp": dp, "tensor": t}

    x_next, x_prev = dev_d(1, 0), dev_d(NX - 1, 0)
    y_other = dev_d(0, 1)
    sib = dev_t(0, 0, 1)
    h_other = dev_t(1, 0)
    z_next, z_prev = dev_t(0, 1), dev_t(0, NZ - 1)
    sent = []

    def send(src, dst, ssem, rsem, device):
        copy = pltpu.make_async_remote_copy(
            src_ref=src,
            dst_ref=dst,
            send_sem=ssem,
            recv_sem=rsem,
            device_id=device,
            device_id_type=MESH,
        )
        copy.start()
        sent.append(copy)

    def arrived(dst, ssem, rsem, device):
        pltpu.make_async_remote_copy(
            src_ref=dst,
            dst_ref=dst,
            send_sem=ssem,
            recv_sem=rsem,
            device_id=device,
            device_id_type=MESH,
        ).wait_recv()

    dp_others = [(dx, dy) for dx in (1, 3, 2, 0) for dy in (0, 1) if (dx, dy) != (0, 0)]
    tp_others = [(dh, dz) for dz in (2, 1, 3, 0) for dh in (1, 0) if (dh, dz) != (0, 0)]

    row_others = [(dx, dy, 0) for dx, dy in dp_others]
    row_others += [(dx, dy, 1) for dx, dy in [*dp_others, (0, 0)]]

    loads = [
        pltpu.make_async_copy(wu_hbm, wu, w_sem.at[0]),
        pltpu.make_async_copy(wg_hbm, wg, w_sem.at[1]),
        pltpu.make_async_copy(wd_hbm, wd, w_sem.at[2]),
    ]
    rows_in = pltpu.make_async_copy(x_hbm, x_ref, l_sem.at[0])
    rows_in.start()
    mine = x * NY + y

    barrier = pltpu.get_barrier_semaphore()
    for dx, dy, dh in row_others:
        pl.semaphore_signal(barrier, inc=1, device_id=dev_d(dx, dy, dh), device_id_type=MESH)
    for dh, dz in tp_others:
        if dz == 0:
            continue
        pl.semaphore_signal(barrier, inc=1, device_id=dev_t(dh, dz), device_id_type=MESH)
    pl.semaphore_signal(barrier, inc=1, device_id=sib, device_id_type=MESH)
    rows_in.wait()
    own = pltpu.make_async_copy(
        x_ref.at[:, pl.ds(pl.multiple_of(dp * DS, DS), DS)], xb.at[tp, mine], l_sem.at[1]
    )
    own.start()
    wide = x_ref[...].astype(F32)
    inv = lax.rsqrt(jnp.sum(wide * wide, axis=1, keepdims=True) / D + 1e-05)
    hi = inv.astype(BF16).astype(F32)
    mid = (inv - hi).astype(BF16).astype(F32)
    low = inv - hi - mid
    words[...] = jnp.zeros((8, 512), jnp.int32)
    words[:, 0:448] = kb_ref[...]
    lane = lax.broadcasted_iota(jnp.int32, (8, 128), 1)
    scale = jnp.where(lane == 112, hi, jnp.where(lane == 113, mid, low))
    scale = jnp.where((lane >= 112) & (lane < 115), scale, 0.0)
    for t in range(16):
        tile, start = divmod(28 * t, 128)
        piece = words[:, tile * 128 : tile * 128 + 128]
        if start:
            piece = pltpu.roll(piece, 128 - start, 1)
        if start + 28 > 128:
            after = pltpu.roll(words[:, tile * 128 + 128 : tile * 128 + 256], 128 - start, 1)
            piece = jnp.where(lane < 128 - start, piece, after)
        taken = jnp.zeros((8, 128), jnp.int32)
        for j in range(4):
            byte = (piece >> (8 * j)) & 255
            if j:
                byte = pltpu.roll(byte, 28 * j, 1)
            taken = jnp.where((lane >= 28 * j) & (lane < 28 * j + 28), byte, taken)
        slot = (taken.astype(F32) + scale).astype(BF16)
        xb[tp, 8 + t // 8, :, (t % 8) * 128 : (t % 8) * 128 + 128] = slot
    pl.semaphore_wait(barrier, len(row_others) + 7)

    for i, (dx, dy, dh) in enumerate(row_others):
        there = lax.rem(y + dy, NY) * NX + lax.rem(x + dx, NX)
        send(
            x_ref.at[:, pl.ds(pl.multiple_of(there * DS, DS), DS)],
            xb.at[tp, mine],
            a_send.at[i],
            a_recv.at[h, mine],
            dev_d(dx, dy, dh),
        )
    send(xb.at[tp, pl.ds(8, 2)], xb.at[tp, pl.ds(8, 2)], k_sem.at[0], k_sem.at[1], h_other)
    for load in loads:
        load.start()
    row = lax.broadcasted_iota(jnp.int32, (128, FU), 0)
    col = lax.broadcasted_iota(jnp.int32, (128, FU), 1)
    place = ((col & 31) >> 3) * 28 + (col >> 5)
    spread[...] = jnp.where(row == place, 1.0, 0.0).astype(BF16)
    count = [0]

    def push(t, device):
        send(xb.at[t], xb.at[t], x_send.at[count[0]], x_recv.at[t], device)
        count[0] += 1

    def here(t):
        arrived(xb.at[t], x_send.at[0], x_recv.at[t], sib)

    z1, z3, z2 = lax.rem(z + 1, NZ), lax.rem(z + 3, NZ), lax.rem(z + 2, NZ)
    hh = 1 - h
    across = t_of(hh, z, c)
    own.wait()
    for there in range(2):
        for i, (dx, dy, dh) in enumerate(row_others):
            if dh == there:
                g = lax.rem(x + dx, NX) * NY + lax.rem(y + dy, NY)
                t = across if dh else tp
                arrived(xb.at[t, g], a_send.at[i], a_recv.at[lax.rem(h + dh, NH), g], h_other)
        if there == 0:
            push(tp, sib)
            push(tp, z_next)
            push(tp, z_prev)
    arrived(xb.at[across, pl.ds(8, 2)], k_sem.at[0], k_sem.at[1], h_other)
    push(across, sib)
    push(across, z_next)
    push(across, z_prev)

    def gather_near():
        a, b = t_of(h, z1, c), t_of(h, z3, c)
        e, f = t_of(hh, z1, c), t_of(hh, z3, c)
        here(a)
        push(a, z_prev)
        push(a, sib)
        here(b)
        push(b, sib)
        here(f)
        push(f, z_next)
        push(f, sib)
        here(e)
        push(e, sib)

    def gather_far():
        a, b = t_of(h, z2, c), t_of(hh, z2, c)
        here(a)
        push(a, sib)
        here(b)
        push(b, sib)

    xn1, xp1, xf = lax.rem(x + 1, NX), lax.rem(x + 3, NX), lax.rem(x + 2, NX)

    def matmul(k):
        zz = lax.rem(z + OFFSETS[k], NZ)
        here(t_of(0, zz, 1 - c))
        here(t_of(1, zz, 1 - c))
        blocks = [t_of(a, zz, b) for a in range(2) for b in range(2)]
        gain = gain_ref[...].astype(F32).reshape(1, DS)
        for g in range(8):
            for i in range(4):
                v = xb[blocks[i], g].astype(F32) * gain
                xn[pl.ds(g * 32 + i * 8, 8), :] = v
        lhs = xn[...].astype(BF16)
        if k == 0:
            loads[0].wait()
        acc = jnp.dot(lhs, wu[...], preferred_element_type=F32).astype(BF16)
        for g in range(8):
            for i in range(2):
                lo = g * 32 + i * 16
                pu[k, g % 2, g // 2, i] = acc[lo : lo + 16]
        send(pu.at[k, 1 - y], u_y.at[k], u_send.at[k, 0], u_done.at[k, 0], y_other)
        if k == 0:
            loads[1].wait()
        acc = jnp.dot(lhs, wg[...], preferred_element_type=F32).astype(BF16)
        for g in range(8):
            pg[k, g // 2, g % 2] = acc[g * 32 : g * 32 + 32]
        send(pg.at[k, xf, 0], g_relay.at[k, 0], g_send.at[k, 0], g_done.at[k, 0], x_next)
        send(pg.at[k, xf, 1], g_relay.at[k, 1], g_send.at[k, 1], g_done.at[k, 1], x_prev)
        send(pg.at[k, xn1, 1], g_recv.at[k, 0, 1], g_send.at[k, 3], g_done.at[k, 3], x_next)
        send(pg.at[k, xp1, 0], g_recv.at[k, 1, 0], g_send.at[k, 4], g_done.at[k, 4], x_prev)

    def gate_relay(k):
        arrived(g_relay.at[k, 0], g_send.at[k, 0], g_done.at[k, 0], x_next)
        v = pg[k, xn1, 0].astype(F32) + g_relay[k, 0].astype(F32)
        pg[k, xn1, 0] = v.astype(BF16)
        send(pg.at[k, xn1, 0], g_recv.at[k, 0, 0], g_send.at[k, 2], g_done.at[k, 2], x_next)
        arrived(g_relay.at[k, 1], g_send.at[k, 1], g_done.at[k, 1], x_prev)
        v = pg[k, xp1, 1].astype(F32) + g_relay[k, 1].astype(F32)
        pg[k, xp1, 1] = v.astype(BF16)
        send(pg.at[k, xp1, 1], g_recv.at[k, 1, 1], g_send.at[k, 5], g_done.at[k, 5], x_prev)

    def gate_over_x(k, yy):
        return (
            pg[k, x, yy].astype(F32) + g_recv[k, 0, yy].astype(F32) + g_recv[k, 1, yy].astype(F32)
        )

    def gate_y(k):
        arrived(g_recv.at[k, 0, 1], g_send.at[k, 3], g_done.at[k, 3], x_next)
        arrived(g_recv.at[k, 1, 0], g_send.at[k, 4], g_done.at[k, 4], x_prev)
        arrived(g_recv.at[k, 0, 0], g_send.at[k, 2], g_done.at[k, 2], x_next)
        arrived(g_recv.at[k, 1, 1], g_send.at[k, 5], g_done.at[k, 5], x_prev)
        ysend[k] = gate_over_x(k, 1 - y).astype(BF16)
        send(ysend.at[k], yrecv.at[k], g_send.at[k, 6], g_done.at[k, 6], y_other)

    def up_over_y(k):
        arrived(u_y.at[k], u_send.at[k, 0], u_done.at[k, 0], y_other)
        for xx in (xf, xn1, xp1, x):
            v = pu[k, y, xx].astype(F32) + u_y[k, xx].astype(F32)
            pu[k, y, xx] = v.astype(BF16)
            if xx is xf:
                send(pu.at[k, y, xf, 0], u_relay.at[k, 0], u_send.at[k, 1], u_done.at[k, 1], x_next)
                send(pu.at[k, y, xf, 1], u_relay.at[k, 1], u_send.at[k, 2], u_done.at[k, 2], x_prev)
            if xx is xn1:
                send(
                    pu.at[k, y, xx, 1], u_recv.at[k, 0, 1], u_send.at[k, 3], u_done.at[k, 3], x_next
                )
            if xx is xp1:
                send(
                    pu.at[k, y, xx, 0], u_recv.at[k, 1, 0], u_send.at[k, 4], u_done.at[k, 4], x_prev
                )

    def up_relay(k):
        arrived(u_relay.at[k, 0], u_send.at[k, 1], u_done.at[k, 1], x_next)
        v = pu[k, y, xn1, 0].astype(F32) + u_relay[k, 0].astype(F32)
        pu[k, y, xn1, 0] = v.astype(BF16)
        send(pu.at[k, y, xn1, 0], u_recv.at[k, 0, 0], u_send.at[k, 5], u_done.at[k, 5], x_next)
        arrived(u_relay.at[k, 1], u_send.at[k, 2], u_done.at[k, 2], x_prev)
        v = pu[k, y, xp1, 1].astype(F32) + u_relay[k, 1].astype(F32)
        pu[k, y, xp1, 1] = v.astype(BF16)
        send(pu.at[k, y, xp1, 1], u_recv.at[k, 1, 1], u_send.at[k, 6], u_done.at[k, 6], x_prev)

    def hidden(k):
        zz = lax.rem(z + OFFSETS[k], NZ)
        lanes = pl.ds(pl.multiple_of(lax.rem(tp, 8) * 128, 128), 128)
        slots = jnp.concatenate(
            [
                xb[t_of(a, zz, b), 8 + lax.div(tp, 8), :, lanes].astype(F32)
                for a in range(2)
                for b in range(2)
            ],
            axis=0,
        )
        lane = lax.broadcasted_iota(jnp.int32, (32, 128), 1)
        inv = jnp.sum(
            jnp.where((lane >= 112) & (lane < 115), slots, 0.0), axis=1, keepdims=True
        )
        byte = jnp.dot(slots.astype(BF16), spread[...], preferred_element_type=F32)
        unit = lax.broadcasted_iota(jnp.int32, (32, FU), 1)
        bit = (byte.astype(jnp.int32) >> (unit & 7)) & 1
        keep = 2.0 * bit.astype(F32)
        arrived(yrecv.at[k], g_send.at[k, 6], g_done.at[k, 6], y_other)
        gate = (gate_over_x(k, y) + yrecv[k].astype(F32)) * inv
        arrived(u_recv.at[k, 0, 1], u_send.at[k, 3], u_done.at[k, 3], x_next)
        arrived(u_recv.at[k, 1, 0], u_send.at[k, 4], u_done.at[k, 4], x_prev)
        arrived(u_recv.at[k, 0, 0], u_send.at[k, 5], u_done.at[k, 5], x_next)
        arrived(u_recv.at[k, 1, 1], u_send.at[k, 6], u_done.at[k, 6], x_prev)
        up = pu[k, y, x].astype(F32) + u_recv[k, 0].astype(F32) + u_recv[k, 1].astype(F32)
        up = up.reshape(32, FU) * inv
        hid[k, x, y] = (gate / (1.0 + jnp.exp(-gate)) * up * keep).astype(BF16)
        for i, device in enumerate((x_next, x_prev, y_other)):
            send(hid.at[k, x, y], hid.at[k, x, y], h_send.at[k, i], h_recv.at[k, mine], device)

    def h_here(k, xx, yy):
        arrived(hid.at[k, xx, yy], h_send.at[k, 0], h_recv.at[k, xx * NY + yy], x_next)

    def pass_y(k):
        h_here(k, x, 1 - y)
        for i, device in enumerate((x_next, x_prev)):
            send(
                hid.at[k, x, 1 - y],
                hid.at[k, x, 1 - y],
                h_send.at[k, 3 + i],
                h_recv.at[k, x * NY + 1 - y],
                device,
            )

    def pass_x(k):
        h_here(k, xp1, 0)
        send(
            hid.at[k, xp1, 0], hid.at[k, xp1, 0], h_send.at[k, 5], h_recv.at[k, xp1 * NY], x_next
        )
        h_here(k, xn1, 1)
        send(
            hid.at[k, xn1, 1],
            hid.at[k, xn1, 1],
            h_send.at[k, 6],
            h_recv.at[k, xn1 * NY + 1],
            x_prev,
        )

    def down(k):
        h_here(k, xp1, 1)
        h_here(k, xn1, 0)
        h_here(k, xf, 0)
        h_here(k, xf, 1)
        if k == 0:
            loads[2].wait()
        lhs = hid[k].reshape(256, FU)
        acc = jnp.dot(lhs, wd[...], preferred_element_type=F32).astype(BF16)
        for g in range(8):
            for s in range(2):
                osum[k, s, g] = acc[g * 32 + s * 16 : g * 32 + s * 16 + 16]
        send(osum.at[k, 1 - c], orecv.at[k], o_send.at[k], o_recv.at[k], sib)

    def to_owners(k):
        zz = lax.rem(z + OFFSETS[k], NZ)
        arrived(orecv.at[k], o_send.at[k], o_recv.at[k], sib)
        fsend[k] = (osum[k, c].astype(F32) + orecv[k].astype(F32)).astype(BF16)
        here_index = h * NZ + z
        for i, (dh, dz) in enumerate(tp_others):
            g = lax.rem(z + dz, NZ) * NY + lax.rem(h + dh, NH)
            send(
                fsend.at[k, g],
                frecv.at[here_index, zz],
                f_send.at[k, i],
                f_recv.at[here_index, zz],
                dev_t(dh, dz),
            )

    matmul(0)
    gather_near()
    gate_relay(0)
    matmul(2)
    matmul(1)
    gate_y(0)
    up_over_y(0)
    gather_far()
    matmul(3)
    up_over_y(2)
    gate_relay(3)
    up_relay(0)
    up_over_y(1)
    gate_relay(1)
    gate_relay(2)
    hidden(0)
    up_relay(1)
    up_relay(2)
    gate_y(1)
    gate_y(2)
    up_over_y(3)
    gate_y(3)
    pass_y(0)
    hidden(1)
    hidden(2)
    pass_x(0)
    pass_y(1)
    up_relay(3)
    pass_y(2)
    down(0)
    pass_x(1)
    hidden(3)
    pass_x(2)
    to_owners(0)
    down(1)
    pass_y(3)
    to_owners(1)
    down(2)
    pass_x(3)
    to_owners(2)
    down(3)
    to_owners(3)

    late = len(sent) - 7
    for copy in sent[:late]:
        copy.wait_send()
    for k in range(4):
        zz = lax.rem(z + OFFSETS[k], NZ)
        total = fsend[k, z * NY + h].astype(F32)
        res = jnp.concatenate(
            [xb[t_of(c, zz, b), z * NY + h].astype(F32) for b in range(2)], axis=0
        )
        total = total + res
        for i, (dh, dz) in enumerate(tp_others):
            src = lax.rem(h + dh, NH) * NZ + lax.rem(z + dz, NZ)
            arrived(frecv.at[src, zz], f_send.at[0, i], f_recv.at[src, zz], dev_t(dh, dz))
            total = total + frecv[src, zz].astype(F32)
        rounded = total.astype(BF16)
        out_ref[pl.ds(pl.multiple_of(zz * 16, 16), 16), :] = rounded
    wide = out_ref[...].astype(F32)
    wide = wide * wide
    folded = wide[:, 0:128]
    for i in range(1, 8):
        folded = folded + wide[:, i * 128 : (i + 1) * 128]
    rowsum = jnp.sum(folded.T, axis=0, keepdims=True)
    csend[:, 0:64] = jnp.broadcast_to(rowsum, (8, 64))
    csend[:, 64:128] = jnp.zeros((8, 64), F32)
    for i, (dx, dy) in enumerate(dp_others):
        send(csend, crecv.at[mine], c_send.at[i], c_recv.at[mine], dev_d(dx, dy))
    total = csend[...]
    for i, (dx, dy) in enumerate(dp_others):
        g = lax.rem(x + dx, NX) * NY + lax.rem(y + dy, NY)
        arrived(crecv.at[g], c_send.at[i], c_recv.at[g], dev_d(dx, dy))
        total = total + crecv[g]
    rc_ref[...] = total[0, 0:64] / D
    for copy in sent[late:]:
        copy.wait_send()


def on_device(saved_input, keep_bits, norm_gain, gate_weight, up_weight, down_weight):
    vmem = pl.BlockSpec(memory_space=pltpu.VMEM)
    hbm = pl.BlockSpec(memory_space=pltpu.HBM)
    dma = pltpu.SemaphoreType.DMA
    out, check = pl.pallas_call(
        kernel,
        out_shape=(
            jax.ShapeDtypeStruct((64, DS), BF16),
            jax.ShapeDtypeStruct((64,), F32),
        ),
        in_specs=[hbm, vmem, vmem, hbm, hbm, hbm],
        out_specs=(vmem, vmem),
        scratch_shapes=[
            pltpu.VMEM((DS, FU), BF16),
            pltpu.VMEM((DS, FU), BF16),
            pltpu.VMEM((FU, DS), BF16),
            pltpu.VMEM((128, FU), BF16),
            pltpu.VMEM((8, 512), jnp.int32),
            pltpu.VMEM((8, D), BF16),
            pltpu.VMEM((16, 10, 8, DS), BF16),
            pltpu.VMEM((256, DS), F32),
            pltpu.VMEM((4, 4, 2, 32, FU), BF16),
            pltpu.VMEM((4, 2, 4, 2, 16, FU), BF16),
            pltpu.VMEM((4, 2, 32, FU), BF16),
            pltpu.VMEM((4, 2, 2, 32, FU), BF16),
            pltpu.VMEM((4, 2, 16, FU), BF16),
            pltpu.VMEM((4, 2, 2, 16, FU), BF16),
            pltpu.VMEM((4, 4, 2, 16, FU), BF16),
            pltpu.VMEM((4, 32, FU), BF16),
            pltpu.VMEM((4, 32, FU), BF16),
            pltpu.VMEM((4, 4, 2, 32, FU), BF16),
            pltpu.VMEM((4, 2, 8, 16, DS), BF16),
            pltpu.VMEM((4, 8, 16, DS), BF16),
            pltpu.VMEM((4, 8, 16, DS), BF16),
            pltpu.VMEM((8, 4, 16, DS), BF16),
            pltpu.VMEM((8, 128), F32),
            pltpu.VMEM((8, 8, 128), F32),
            dma((3,)),
            dma((2,)),
            dma((15,)),
            dma((2, 8)),
            dma((2,)),
            dma((14,)),
            dma((16,)),
            dma((4, 7)),
            dma((4, 7)),
            dma((4, 7)),
            dma((4, 7)),
            dma((4, 7)),
            dma((4, 8)),
            dma((4,)),
            dma((4,)),
            dma((4, 7)),
            dma((8, 4)),
            dma((7,)),
            dma((8,)),
        ],
        compiler_params=pltpu.CompilerParams(
            collective_id=0, has_side_effects=True, vmem_limit_bytes=54000 * 1024
        ),
        name="block",
    )(saved_input, keep_bits, norm_gain, gate_weight, up_weight, down_weight)
    return out, check


def solution(mesh):
    both = ("dp", "tensor")
    return jax.shard_map(
        on_device,
        mesh=mesh,
        in_specs=(
            P(both, None),
            P(both, None),
            P("dp"),
            P("dp", "tensor"),
            P("dp", "tensor"),
            P("tensor", "dp"),
        ),
        out_specs=(P("tensor", "dp"), P("tensor")),
        check_vma=False,
    )
```

```python
import jax
import jax.numpy as jnp
from jax import lax
from jax.experimental import pallas as pl
from jax.experimental.pallas import tpu as pltpu
from jax.sharding import PartitionSpec as P

D = 8192
DS = 1024
FU = 896
MESH = pl.DeviceIdType.MESH
F32 = jnp.float32
BF16 = jnp.bfloat16
NX, NY, NH, NZ = 4, 2, 2, 4
OFFSETS = (0, 1, 3, 2)


def kernel(
    x_hbm,
    kb_hbm,
    gain_hbm,
    wg_hbm,
    wu_hbm,
    wd_hbm,
    out_ref,
    rc_ref,
    wg,
    wu,
    wd,
    spread,
    words,
    kb_ref,
    gain_ref,
    x_ref,
    xb,
    xn,
    pg,
    pu,
    g_relay,
    g_recv,
    u_relay,
    u_recv,
    u_y,
    ysend,
    yrecv,
    hid,
    osum,
    orecv,
    fsend,
    frecv,
    obuf,
    sq,
    csend,
    crecv,
    w_sem,
    l_sem,
    a_send,
    a_recv,
    k_sem,
    x_send,
    x_recv,
    g_send,
    g_done,
    u_send,
    u_done,
    h_send,
    h_recv,
    o_send,
    o_recv,
    f_send,
    f_recv,
    c_send,
    c_recv,
):
    dp = lax.axis_index("dp")
    tp = lax.axis_index("tensor")
    x, y = lax.rem(dp, NX), lax.div(dp, NX)
    c, z, h = lax.rem(tp, 2), lax.rem(lax.div(tp, 2), NZ), lax.div(tp, 2 * NZ)

    def t_of(hh, zz, cc):
        return (hh * NZ + zz) * 2 + cc

    def dev_d(dx, dy, dh=0):
        d = lax.rem(y + dy, NY) * NX + lax.rem(x + dx, NX)
        return {"dp": d, "tensor": t_of(lax.rem(h + dh, NH), z, c)}

    def dev_t(dh, dz, dc=0):
        t = t_of(lax.rem(h + dh, NH), lax.rem(z + dz, NZ), lax.rem(c + dc, 2))
        return {"dp": dp, "tensor": t}

    x_next, x_prev = dev_d(1, 0), dev_d(NX - 1, 0)
    y_other = dev_d(0, 1)
    sib = dev_t(0, 0, 1)
    h_other = dev_t(1, 0)
    z_next, z_prev = dev_t(0, 1), dev_t(0, NZ - 1)
    sent = []

    def send(src, dst, ssem, rsem, device):
        copy = pltpu.make_async_remote_copy(
            src_ref=src,
            dst_ref=dst,
            send_sem=ssem,
            recv_sem=rsem,
            device_id=device,
            device_id_type=MESH,
        )
        copy.start()
        sent.append(copy)

    def arrived(dst, ssem, rsem, device):
        pltpu.make_async_remote_copy(
            src_ref=dst,
            dst_ref=dst,
            send_sem=ssem,
            recv_sem=rsem,
            device_id=device,
            device_id_type=MESH,
        ).wait_recv()

    dp_others = [(dx, dy) for dx in (1, 3, 2, 0) for dy in (0, 1) if (dx, dy) != (0, 0)]
    tp_others = [(dh, dz) for dz in (2, 1, 3, 0) for dh in (1, 0) if (dh, dz) != (0, 0)]

    row_others = [(dx, dy, 0) for dx, dy in dp_others]
    row_others += [(dx, dy, 1) for dx, dy in [*dp_others, (0, 0)]]

    loads = [
        pltpu.make_async_copy(wu_hbm, wu, w_sem.at[0]),
        pltpu.make_async_copy(wg_hbm, wg, w_sem.at[1]),
        pltpu.make_async_copy(wd_hbm, wd, w_sem.at[2]),
    ]
    rows_in = [
        pltpu.make_async_copy(x_hbm, x_ref, l_sem.at[0]),
        pltpu.make_async_copy(kb_hbm, kb_ref, l_sem.at[2]),
        pltpu.make_async_copy(gain_hbm, gain_ref, l_sem.at[3]),
    ]
    for load in rows_in:
        load.start()
    mine = x * NY + y

    barrier = pltpu.get_barrier_semaphore()
    for dx, dy, dh in row_others:
        pl.semaphore_signal(barrier, inc=1, device_id=dev_d(dx, dy, dh), device_id_type=MESH)
    for dh, dz in tp_others:
        if dz == 0:
            continue
        pl.semaphore_signal(barrier, inc=1, device_id=dev_t(dh, dz), device_id_type=MESH)
    pl.semaphore_signal(barrier, inc=1, device_id=sib, device_id_type=MESH)
    for load in rows_in:
        load.wait()
    own = pltpu.make_async_copy(
        x_ref.at[:, pl.ds(pl.multiple_of(dp * DS, DS), DS)], xb.at[tp, mine], l_sem.at[1]
    )
    own.start()
    wide = x_ref[...].astype(F32)
    inv = lax.rsqrt(jnp.sum(wide * wide, axis=1, keepdims=True) / D + 1e-05)
    hi = inv.astype(BF16).astype(F32)
    mid = (inv - hi).astype(BF16).astype(F32)
    low = inv - hi - mid
    words[...] = jnp.zeros((8, 512), jnp.int32)
    words[:, 0:448] = kb_ref[...]
    lane = lax.broadcasted_iota(jnp.int32, (8, 128), 1)
    scale = jnp.where(lane == 112, hi, jnp.where(lane == 113, mid, low))
    scale = jnp.where((lane >= 112) & (lane < 115), scale, 0.0)
    for t in range(16):
        tile, start = divmod(28 * t, 128)
        piece = words[:, tile * 128 : tile * 128 + 128]
        if start:
            piece = pltpu.roll(piece, 128 - start, 1)
        if start + 28 > 128:
            after = pltpu.roll(words[:, tile * 128 + 128 : tile * 128 + 256], 128 - start, 1)
            piece = jnp.where(lane < 128 - start, piece, after)
        taken = jnp.zeros((8, 128), jnp.int32)
        for j in range(4):
            byte = (piece >> (8 * j)) & 255
            if j:
                byte = pltpu.roll(byte, 28 * j, 1)
            taken = jnp.where((lane >= 28 * j) & (lane < 28 * j + 28), byte, taken)
        slot = (taken.astype(F32) + scale).astype(BF16)
        xb[tp, 8 + t // 8, :, (t % 8) * 128 : (t % 8) * 128 + 128] = slot
    pl.semaphore_wait(barrier, len(row_others) + 7)

    for i, (dx, dy, dh) in enumerate(row_others):
        there = lax.rem(y + dy, NY) * NX + lax.rem(x + dx, NX)
        send(
            x_ref.at[:, pl.ds(pl.multiple_of(there * DS, DS), DS)],
            xb.at[tp, mine],
            a_send.at[i],
            a_recv.at[h, mine],
            dev_d(dx, dy, dh),
        )
    send(xb.at[tp, pl.ds(8, 2)], xb.at[tp, pl.ds(8, 2)], k_sem.at[0], k_sem.at[1], h_other)
    for load in loads:
        load.start()
    row = lax.broadcasted_iota(jnp.int32, (128, FU), 0)
    col = lax.broadcasted_iota(jnp.int32, (128, FU), 1)
    place = ((col & 31) >> 3) * 28 + (col >> 5)
    spread[...] = jnp.where(row == place, 1.0, 0.0).astype(BF16)
    count = [0, 0]
    xs, ks = pl.ds(0, 8), pl.ds(8, 2)

    def push(t, device, part=0):
        cells = xb.at[t, ks if part else xs]
        send(cells, cells, x_send.at[part, count[part]], x_recv.at[part, t], device)
        count[part] += 1

    def here(t, part=0):
        cells = xb.at[t, ks if part else xs]
        arrived(cells, x_send.at[part, 0], x_recv.at[part, t], sib)

    z1, z3, z2 = lax.rem(z + 1, NZ), lax.rem(z + 3, NZ), lax.rem(z + 2, NZ)
    hh = 1 - h
    across = t_of(hh, z, c)
    own.wait()
    for there in range(2):
        for i, (dx, dy, dh) in enumerate(row_others):
            if dh == there:
                g = lax.rem(x + dx, NX) * NY + lax.rem(y + dy, NY)
                t = across if dh else tp
                arrived(xb.at[t, g], a_send.at[i], a_recv.at[lax.rem(h + dh, NH), g], h_other)
        if there == 0:
            push(tp, sib)
            push(tp, z_next)
            push(tp, z_prev)
    push(across, sib)
    push(across, z_next)
    push(across, z_prev)
    push(tp, sib, 1)
    push(tp, z_next, 1)
    push(tp, z_prev, 1)
    arrived(xb.at[across, ks], k_sem.at[0], k_sem.at[1], h_other)
    push(across, sib, 1)
    push(across, z_next, 1)
    push(across, z_prev, 1)

    def gather_near(part):
        a, b = t_of(h, z1, c), t_of(h, z3, c)
        e, f = t_of(hh, z1, c), t_of(hh, z3, c)
        here(a, part)
        push(a, z_prev, part)
        push(a, sib, part)
        here(b, part)
        push(b, sib, part)
        here(f, part)
        push(f, z_next, part)
        push(f, sib, part)
        here(e, part)
        push(e, sib, part)

    def gather_far(part):
        a, b = t_of(h, z2, c), t_of(hh, z2, c)
        here(a, part)
        push(a, sib, part)
        here(b, part)
        push(b, sib, part)

    def source(k):
        return 1 - c if k % 2 == 0 else c, lax.rem(z + OFFSETS[k // 2], NZ)

    xn1, xp1, xf = lax.rem(x + 1, NX), lax.rem(x + 3, NX), lax.rem(x + 2, NX)

    def matmul(k):
        hs, zz = source(k)
        here(t_of(hs, zz, 1 - c))
        gain = gain_ref[...].astype(F32).reshape(1, DS)
        for g in range(8):
            for i in range(2):
                v = xb[t_of(hs, zz, i), g].astype(F32) * gain
                xn[pl.ds(g * 16 + i * 8, 8), :] = v
        lhs = xn[...].astype(BF16)
        if k == 0:
            loads[0].wait()
        acc = jnp.dot(lhs, wu[...], preferred_element_type=F32)
        for g in range(8):
            for i in range(2):
                lo = g * 16 + i * 8
                pu[k, g % 2, g // 2, i] = acc[lo : lo + 8].astype(BF16)
        send(pu.at[k, 1 - y], u_y.at[k], u_send.at[k, 0], u_done.at[k, 0], y_other)
        if k == 0:
            loads[1].wait()
        acc = jnp.dot(lhs, wg[...], preferred_element_type=F32).astype(BF16)
        for g in range(8):
            pg[k, g // 2, g % 2] = acc[g * 16 : g * 16 + 16]
        send(pg.at[k, xf, 0], g_relay.at[k, 0], g_send.at[k, 0], g_done.at[k, 0], x_next)
        send(pg.at[k, xf, 1], g_relay.at[k, 1], g_send.at[k, 1], g_done.at[k, 1], x_prev)
        send(pg.at[k, xn1, 1], g_recv.at[k, 0, 1], g_send.at[k, 3], g_done.at[k, 3], x_next)
        send(pg.at[k, xp1, 0], g_recv.at[k, 1, 0], g_send.at[k, 4], g_done.at[k, 4], x_prev)

    def gate_relay(k):
        arrived(g_relay.at[k, 0], g_send.at[k, 0], g_done.at[k, 0], x_next)
        v = pg[k, xn1, 0].astype(F32) + g_relay[k, 0].astype(F32)
        pg[k, xn1, 0] = v.astype(BF16)
        send(pg.at[k, xn1, 0], g_recv.at[k, 0, 0], g_send.at[k, 2], g_done.at[k, 2], x_next)
        arrived(g_relay.at[k, 1], g_send.at[k, 1], g_done.at[k, 1], x_prev)
        v = pg[k, xp1, 1].astype(F32) + g_relay[k, 1].astype(F32)
        pg[k, xp1, 1] = v.astype(BF16)
        send(pg.at[k, xp1, 1], g_recv.at[k, 1, 1], g_send.at[k, 5], g_done.at[k, 5], x_prev)

    def gate_over_x(k, yy):
        return (
            pg[k, x, yy].astype(F32) + g_recv[k, 0, yy].astype(F32) + g_recv[k, 1, yy].astype(F32)
        )

    def gate_y(k):
        arrived(g_recv.at[k, 0, 1], g_send.at[k, 3], g_done.at[k, 3], x_next)
        arrived(g_recv.at[k, 1, 0], g_send.at[k, 4], g_done.at[k, 4], x_prev)
        arrived(g_recv.at[k, 0, 0], g_send.at[k, 2], g_done.at[k, 2], x_next)
        arrived(g_recv.at[k, 1, 1], g_send.at[k, 5], g_done.at[k, 5], x_prev)
        ysend[k] = gate_over_x(k, 1 - y).astype(BF16)
        send(ysend.at[k], yrecv.at[k], g_send.at[k, 6], g_done.at[k, 6], y_other)

    def up_over_y(k):
        arrived(u_y.at[k], u_send.at[k, 0], u_done.at[k, 0], y_other)
        for xx in (xf, xn1, xp1, x):
            v = pu[k, y, xx].astype(F32) + u_y[k, xx].astype(F32)
            pu[k, y, xx] = v.astype(BF16)
            if xx is xf:
                send(pu.at[k, y, xf, 0], u_relay.at[k, 0], u_send.at[k, 1], u_done.at[k, 1], x_next)
                send(pu.at[k, y, xf, 1], u_relay.at[k, 1], u_send.at[k, 2], u_done.at[k, 2], x_prev)
            if xx is xn1:
                send(
                    pu.at[k, y, xx, 1], u_recv.at[k, 0, 1], u_send.at[k, 3], u_done.at[k, 3], x_next
                )
            if xx is xp1:
                send(
                    pu.at[k, y, xx, 0], u_recv.at[k, 1, 0], u_send.at[k, 4], u_done.at[k, 4], x_prev
                )

    def up_relay(k):
        arrived(u_relay.at[k, 0], u_send.at[k, 1], u_done.at[k, 1], x_next)
        v = pu[k, y, xn1, 0].astype(F32) + u_relay[k, 0].astype(F32)
        pu[k, y, xn1, 0] = v.astype(BF16)
        send(pu.at[k, y, xn1, 0], u_recv.at[k, 0, 0], u_send.at[k, 5], u_done.at[k, 5], x_next)
        arrived(u_relay.at[k, 1], u_send.at[k, 2], u_done.at[k, 2], x_prev)
        v = pu[k, y, xp1, 1].astype(F32) + u_relay[k, 1].astype(F32)
        pu[k, y, xp1, 1] = v.astype(BF16)
        send(pu.at[k, y, xp1, 1], u_recv.at[k, 1, 1], u_send.at[k, 6], u_done.at[k, 6], x_prev)

    def hidden(k):
        hs, zz = source(k)
        here(t_of(hs, zz, 1 - c), 1)
        lanes = pl.ds(pl.multiple_of(lax.rem(tp, 8) * 128, 128), 128)
        slots = [xb[t_of(hs, zz, i), 8 + lax.div(tp, 8), :, lanes].astype(F32) for i in range(2)]
        slots = jnp.concatenate(slots, axis=0)
        lane = lax.broadcasted_iota(jnp.int32, (16, 128), 1)
        inv = jnp.sum(
            jnp.where((lane >= 112) & (lane < 115), slots, 0.0), axis=1, keepdims=True
        )
        byte = jnp.dot(slots.astype(BF16), spread[...], preferred_element_type=F32)
        unit = lax.broadcasted_iota(jnp.int32, (16, FU), 1)
        bit = (byte.astype(jnp.int32) >> (unit & 7)) & 1
        keep = 2.0 * bit.astype(F32)
        arrived(yrecv.at[k], g_send.at[k, 6], g_done.at[k, 6], y_other)
        gate = (gate_over_x(k, y) + yrecv[k].astype(F32)) * inv
        arrived(u_recv.at[k, 0, 1], u_send.at[k, 3], u_done.at[k, 3], x_next)
        arrived(u_recv.at[k, 1, 0], u_send.at[k, 4], u_done.at[k, 4], x_prev)
        arrived(u_recv.at[k, 0, 0], u_send.at[k, 5], u_done.at[k, 5], x_next)
        arrived(u_recv.at[k, 1, 1], u_send.at[k, 6], u_done.at[k, 6], x_prev)
        up = pu[k, y, x].astype(F32) + u_recv[k, 0].astype(F32) + u_recv[k, 1].astype(F32)
        up = up.reshape(16, FU) * inv
        hid[k, x, y] = (gate / (1.0 + jnp.exp(-gate)) * up * keep).astype(BF16)
        for i, device in enumerate((x_next, x_prev, y_other)):
            send(hid.at[k, x, y], hid.at[k, x, y], h_send.at[k, i], h_recv.at[k, mine], device)

    def h_here(k, xx, yy):
        arrived(hid.at[k, xx, yy], h_send.at[k, 0], h_recv.at[k, xx * NY + yy], x_next)

    def pass_y(k):
        h_here(k, x, 1 - y)
        for i, device in enumerate((x_next, x_prev)):
            send(
                hid.at[k, x, 1 - y],
                hid.at[k, x, 1 - y],
                h_send.at[k, 3 + i],
                h_recv.at[k, x * NY + 1 - y],
                device,
            )

    def pass_x(k):
        h_here(k, xp1, 0)
        send(
            hid.at[k, xp1, 0], hid.at[k, xp1, 0], h_send.at[k, 5], h_recv.at[k, xp1 * NY], x_next
        )
        h_here(k, xn1, 1)
        send(
            hid.at[k, xn1, 1],
            hid.at[k, xn1, 1],
            h_send.at[k, 6],
            h_recv.at[k, xn1 * NY + 1],
            x_prev,
        )

    def down(k):
        h_here(k, xp1, 1)
        h_here(k, xn1, 0)
        h_here(k, xf, 0)
        h_here(k, xf, 1)
        if k == 0:
            loads[2].wait()
        acc = jnp.dot(hid[k].reshape(128, FU), wd[...], preferred_element_type=F32)
        i = k // 2
        if k % 2 == 0:
            osum[i] = acc.astype(BF16).reshape(8, 16, DS)
            send(osum.at[i], orecv.at[i], o_send.at[i], o_recv.at[i], sib)
            return
        _, zz = source(k)
        arrived(orecv.at[i], o_send.at[i], o_recv.at[i], sib)
        fsend[i] = (acc.reshape(8, 16, DS) + orecv[i].astype(F32)).astype(BF16)
        for j, (dh, dz) in enumerate(tp_others):
            send(
                fsend.at[i, lax.rem(z + dz, NZ) * NY + lax.rem(h + dh, NH)],
                frecv.at[h * NZ + z, zz],
                f_send.at[i, j],
                f_recv.at[h * NZ + z, zz],
                dev_t(dh, dz),
            )

    matmul(0)
    matmul(1)
    gate_relay(0)
    up_over_y(0)
    gate_relay(1)
    gather_near(0)
    gate_y(0)
    up_relay(0)
    up_over_y(1)
    matmul(2)
    matmul(3)
    gate_y(1)
    up_relay(1)
    matmul(4)
    hidden(0)
    up_over_y(2)
    matmul(5)
    gate_relay(2)
    gate_relay(3)
    gather_near(1)
    up_relay(2)
    gate_relay(5)
    gate_relay(4)
    up_over_y(3)
    gather_far(0)
    up_over_y(4)
    gate_y(2)
    pass_y(0)
    hidden(1)
    matmul(6)
    up_relay(3)
    up_over_y(5)
    gate_y(4)
    pass_x(0)
    gate_y(3)
    pass_y(1)
    up_relay(4)
    gate_y(5)
    hidden(2)
    gate_relay(6)
    up_relay(5)
    gather_far(1)
    matmul(7)
    down(0)
    pass_x(1)
    up_over_y(6)
    hidden(3)
    gate_relay(7)
    pass_y(2)
    hidden(4)
    hidden(5)
    up_over_y(7)
    pass_y(3)
    gate_y(6)
    up_relay(6)
    down(1)
    gate_y(7)
    pass_x(2)
    pass_y(4)
    up_relay(7)
    pass_x(3)
    pass_y(5)
    hidden(6)
    down(2)
    pass_x(4)
    hidden(7)
    down(3)
    pass_y(6)
    pass_x(5)
    pass_y(7)
    down(4)
    pass_x(6)
    down(5)
    pass_x(7)
    down(6)
    down(7)

    late = len(sent) - 7
    for copy in sent[:late]:
        copy.wait_send()
    for k in range(4):
        zz = lax.rem(z + OFFSETS[k], NZ)
        total = fsend[k, z * NY + h].astype(F32)
        res = jnp.concatenate(
            [xb[t_of(c, zz, b), z * NY + h].astype(F32) for b in range(2)], axis=0
        )
        total = total + res
        for i, (dh, dz) in enumerate(tp_others):
            src = lax.rem(h + dh, NH) * NZ + lax.rem(z + dz, NZ)
            arrived(frecv.at[src, zz], f_send.at[0, i], f_recv.at[src, zz], dev_t(dh, dz))
            total = total + frecv[src, zz].astype(F32)
        rounded = total.astype(BF16)
        rows = pl.ds(pl.multiple_of(zz * 16, 16), 16)
        obuf[rows, :] = rounded
        wide = rounded.astype(F32)
        wide = wide * wide
        folded = wide[:, 0:128]
        for i in range(1, 8):
            folded = folded + wide[:, i * 128 : (i + 1) * 128]
        sq[rows, :] = folded
    result = pltpu.make_async_copy(obuf, out_ref, l_sem.at[0])
    result.start()
    rowsum = jnp.sum(sq[...].T, axis=0, keepdims=True)
    csend[:, 0:64] = jnp.broadcast_to(rowsum, (8, 64))
    csend[:, 64:128] = jnp.zeros((8, 64), F32)
    for i, (dx, dy) in enumerate(dp_others):
        send(csend, crecv.at[mine], c_send.at[i], c_recv.at[mine], dev_d(dx, dy))
    total = csend[...]
    for i, (dx, dy) in enumerate(dp_others):
        g = lax.rem(x + dx, NX) * NY + lax.rem(y + dy, NY)
        arrived(crecv.at[g], c_send.at[i], c_recv.at[g], dev_d(dx, dy))
        total = total + crecv[g]
    rc_ref[...] = total[0, 0:64] / D
    result.wait()
    for copy in sent[late:]:
        copy.wait_send()


def on_device(saved_input, keep_bits, norm_gain, gate_weight, up_weight, down_weight):
    vmem = pl.BlockSpec(memory_space=pltpu.VMEM)
    hbm = pl.BlockSpec(memory_space=pltpu.HBM)
    dma = pltpu.SemaphoreType.DMA
    out, check = pl.pallas_call(
        kernel,
        out_shape=(
            jax.ShapeDtypeStruct((64, DS), BF16),
            jax.ShapeDtypeStruct((64,), F32),
        ),
        in_specs=[hbm] * 6,
        out_specs=(hbm, vmem),
        scratch_shapes=[
            pltpu.VMEM((DS, FU), BF16),
            pltpu.VMEM((DS, FU), BF16),
            pltpu.VMEM((FU, DS), BF16),
            pltpu.VMEM((128, FU), BF16),
            pltpu.VMEM((8, 512), jnp.int32),
            pltpu.VMEM((8, 448), jnp.int32),
            pltpu.VMEM((DS,), BF16),
            pltpu.VMEM((8, D), BF16),
            pltpu.VMEM((16, 10, 8, DS), BF16),
            pltpu.VMEM((128, DS), F32),
            pltpu.VMEM((8, 4, 2, 16, FU), BF16),
            pltpu.VMEM((8, 2, 4, 2, 8, FU), BF16),
            pltpu.VMEM((8, 2, 16, FU), BF16),
            pltpu.VMEM((8, 2, 2, 16, FU), BF16),
            pltpu.VMEM((8, 2, 8, FU), BF16),
            pltpu.VMEM((8, 2, 2, 8, FU), BF16),
            pltpu.VMEM((8, 4, 2, 8, FU), BF16),
            pltpu.VMEM((8, 16, FU), BF16),
            pltpu.VMEM((8, 16, FU), BF16),
            pltpu.VMEM((8, 4, 2, 16, FU), BF16),
            pltpu.VMEM((4, 8, 16, DS), BF16),
            pltpu.VMEM((4, 8, 16, DS), BF16),
            pltpu.VMEM((4, 8, 16, DS), BF16),
            pltpu.VMEM((8, 4, 16, DS), BF16),
            pltpu.VMEM((64, DS), BF16),
            pltpu.VMEM((64, 128), F32),
            pltpu.VMEM((8, 128), F32),
            pltpu.VMEM((8, 8, 128), F32),
            dma((3,)),
            dma((4,)),
            dma((15,)),
            dma((2, 8)),
            dma((2,)),
            dma((2, 14)),
            dma((2, 16)),
            dma((8, 7)),
            dma((8, 7)),
            dma((8, 7)),
            dma((8, 7)),
            dma((8, 7)),
            dma((8, 8)),
            dma((4,)),
            dma((4,)),
            dma((4, 7)),
            dma((8, 4)),
            dma((7,)),
            dma((8,)),
        ],
        compiler_params=pltpu.CompilerParams(
            collective_id=0, has_side_effects=True, vmem_limit_bytes=56 * 1024 * 1024
        ),
        name="block",
    )(saved_input, keep_bits, norm_gain, gate_weight, up_weight, down_weight)
    return out, check


def solution(mesh):
    both = ("dp", "tensor")
    return jax.shard_map(
        on_device,
        mesh=mesh,
        in_specs=(
            P(both, None),
            P(both, None),
            P("dp"),
            P("dp", "tensor"),
            P("dp", "tensor"),
            P("tensor", "dp"),
        ),
        out_specs=(P("tensor", "dp"), P("tensor")),
        check_vma=False,
    )
```

```python
import jax
import jax.numpy as jnp
from jax import lax
from jax.experimental import pallas as pl
from jax.experimental.pallas import tpu as pltpu
from jax.sharding import PartitionSpec as P

D = 8192
DS = 1024
FU = 896
MESH = pl.DeviceIdType.MESH
F32 = jnp.float32
BF16 = jnp.bfloat16
NX, NY, NH, NZ = 4, 2, 2, 4
OFFSETS = (0, 1, 3, 2)


def kernel(
    x_hbm,
    kb_hbm,
    gain_hbm,
    wg_hbm,
    wu_hbm,
    wd_hbm,
    out_ref,
    rc_ref,
    wg,
    wu,
    wd,
    spread,
    words,
    kb_ref,
    gain_ref,
    x_ref,
    xb,
    xn,
    pg,
    pu,
    g_relay,
    g_recv,
    u_relay,
    u_recv,
    u_y,
    ysend,
    yrecv,
    hid,
    osum,
    orecv,
    fsend,
    frecv,
    obuf,
    sq,
    csend,
    crecv,
    w_sem,
    l_sem,
    a_send,
    a_recv,
    k_sem,
    x_send,
    x_recv,
    k_recv,
    g_send,
    g_done,
    u_send,
    u_done,
    h_send,
    h_done,
    o_send,
    o_recv,
    f_send,
    f_recv,
    c_send,
    c_recv,
):
    dp = lax.axis_index("dp")
    tp = lax.axis_index("tensor")
    x, y = lax.rem(dp, NX), lax.div(dp, NX)
    c, z, h = lax.rem(tp, 2), lax.rem(lax.div(tp, 2), NZ), lax.div(tp, 2 * NZ)

    def t_of(hh, zz, cc):
        return (hh * NZ + zz) * 2 + cc

    def dev_d(dx, dy, dh=0):
        d = lax.rem(y + dy, NY) * NX + lax.rem(x + dx, NX)
        return {"dp": d, "tensor": t_of(lax.rem(h + dh, NH), z, c)}

    def dev_t(dh, dz, dc=0):
        t = t_of(lax.rem(h + dh, NH), lax.rem(z + dz, NZ), lax.rem(c + dc, 2))
        return {"dp": dp, "tensor": t}

    x_next, x_prev = dev_d(1, 0), dev_d(NX - 1, 0)
    y_other = dev_d(0, 1)
    sib = dev_t(0, 0, 1)
    h_other = dev_t(1, 0)
    z_next, z_prev = dev_t(0, 1), dev_t(0, NZ - 1)

    def send(src, dst, ssem, rsem, device):
        copy = pltpu.make_async_remote_copy(
            src_ref=src,
            dst_ref=dst,
            send_sem=ssem,
            recv_sem=rsem,
            device_id=device,
            device_id_type=MESH,
        )
        copy.start()

    def arrived(dst, rsem, device):
        pltpu.make_async_remote_copy(
            src_ref=dst,
            dst_ref=dst,
            send_sem=rsem,
            recv_sem=rsem,
            device_id=device,
            device_id_type=MESH,
        ).wait_recv()

    def left(src, ssem, device):
        pltpu.make_async_remote_copy(
            src_ref=src,
            dst_ref=src,
            send_sem=ssem,
            recv_sem=ssem,
            device_id=device,
            device_id_type=MESH,
        ).wait_send()

    dp_others = [(dx, dy) for dx in (1, 3, 2, 0) for dy in (0, 1) if (dx, dy) != (0, 0)]
    tp_others = [(dh, dz) for dz in (2, 1, 3, 0) for dh in (1, 0) if (dh, dz) != (0, 0)]

    row_others = [(dx, dy, 0) for dx, dy in dp_others]
    row_others += [(dx, dy, 1) for dx, dy in [*dp_others, (0, 0)]]

    loads = [
        pltpu.make_async_copy(wu_hbm, wu, w_sem.at[0]),
        pltpu.make_async_copy(wg_hbm, wg, w_sem.at[1]),
        pltpu.make_async_copy(wd_hbm, wd, w_sem.at[2]),
    ]
    rows_in = [
        pltpu.make_async_copy(x_hbm, x_ref, l_sem.at[0]),
        pltpu.make_async_copy(kb_hbm, kb_ref, l_sem.at[2]),
        pltpu.make_async_copy(gain_hbm, gain_ref, l_sem.at[3]),
    ]
    for load in rows_in:
        load.start()
    mine = x * NY + y

    barrier = pltpu.get_barrier_semaphore()
    for dx, dy, dh in row_others:
        pl.semaphore_signal(barrier, inc=1, device_id=dev_d(dx, dy, dh), device_id_type=MESH)
    for dh, dz in tp_others:
        if dz == 0:
            continue
        pl.semaphore_signal(barrier, inc=1, device_id=dev_t(dh, dz), device_id_type=MESH)
    pl.semaphore_signal(barrier, inc=1, device_id=sib, device_id_type=MESH)
    for load in rows_in:
        load.wait()
    own = pltpu.make_async_copy(
        x_ref.at[:, pl.ds(pl.multiple_of(dp * DS, DS), DS)], xb.at[tp, mine], l_sem.at[1]
    )
    own.start()
    wide = x_ref[...].astype(F32)
    inv = lax.rsqrt(jnp.sum(wide * wide, axis=1, keepdims=True) / D + 1e-05)
    hi = inv.astype(BF16).astype(F32)
    mid = (inv - hi).astype(BF16).astype(F32)
    low = inv - hi - mid
    words[...] = jnp.zeros((8, 512), jnp.int32)
    words[:, 0:448] = kb_ref[...]
    lane = lax.broadcasted_iota(jnp.int32, (8, 128), 1)
    scale = jnp.where(lane == 112, hi, jnp.where(lane == 113, mid, low))
    scale = jnp.where((lane >= 112) & (lane < 115), scale, 0.0)
    for t in range(16):
        tile, start = divmod(28 * t, 128)
        piece = words[:, tile * 128 : tile * 128 + 128]
        if start:
            piece = pltpu.roll(piece, 128 - start, 1)
        if start + 28 > 128:
            after = pltpu.roll(words[:, tile * 128 + 128 : tile * 128 + 256], 128 - start, 1)
            piece = jnp.where(lane < 128 - start, piece, after)
        taken = jnp.zeros((8, 128), jnp.int32)
        for j in range(4):
            byte = (piece >> (8 * j)) & 255
            if j:
                byte = pltpu.roll(byte, 28 * j, 1)
            taken = jnp.where((lane >= 28 * j) & (lane < 28 * j + 28), byte, taken)
        slot = (taken.astype(F32) + scale).astype(BF16)
        xb[tp, 8 + t // 8, :, (t % 8) * 128 : (t % 8) * 128 + 128] = slot
    pl.semaphore_wait(barrier, len(row_others) + 7)

    for dx, dy, dh in row_others:
        there = lax.rem(y + dy, NY) * NX + lax.rem(x + dx, NX)
        send(
            x_ref.at[:, pl.ds(pl.multiple_of(there * DS, DS), DS)],
            xb.at[tp, mine],
            a_send.at[dh],
            a_recv.at[dh],
            dev_d(dx, dy, dh),
        )
    send(xb.at[tp, pl.ds(8, 2)], xb.at[tp, pl.ds(8, 2)], k_sem.at[0], k_sem.at[1], h_other)
    for load in loads:
        load.start()
    row = lax.broadcasted_iota(jnp.int32, (128, FU), 0)
    col = lax.broadcasted_iota(jnp.int32, (128, FU), 1)
    place = ((col & 31) >> 3) * 28 + (col >> 5)
    spread[...] = jnp.where(row == place, 1.0, 0.0).astype(BF16)
    xs, ks = pl.ds(0, 8), pl.ds(8, 2)

    def push(t, device, part, rsem):
        cells = xb.at[t, ks if part else xs]
        send(cells, cells, x_send.at[part], rsem, device)

    def here(t):
        arrived(xb.at[t, xs], x_recv.at[t], sib)

    def push_x(t, *devices):
        for device in devices:
            push(t, device, 0, x_recv.at[t])

    z1, z3, z2 = lax.rem(z + 1, NZ), lax.rem(z + 3, NZ), lax.rem(z + 2, NZ)
    hh = 1 - h
    across = t_of(hh, z, c)
    own.wait()
    for there in range(2):
        if there == 0:
            arrived(xb.at[tp, pl.ds(0, 7)], a_recv.at[0], y_other)
        else:
            arrived(xb.at[across, pl.ds(0, 8)], a_recv.at[1], h_other)
        push_x(across if there else tp, sib, z_next, z_prev)
    for t in (tp, across):
        if t is across:
            arrived(xb.at[across, ks], k_sem.at[1], h_other)
        push(t, sib, 1, k_recv.at[0])
        push(t, z_next, 1, k_recv.at[1])
        push(t, z_prev, 1, k_recv.at[1])

    near = [t_of(h, z1, c), t_of(h, z3, c), t_of(hh, z3, c), t_of(hh, z1, c)]
    distant = [t_of(h, z2, c), t_of(hh, z2, c)]

    def gather_near(part):
        if part:
            arrived(xb.at[pl.ds(0, 4), ks], k_recv.at[1], z_next)
        for i, t in enumerate(near):
            if not part:
                here(t)
            if i in (0, 2):
                push(t, z_prev if i == 0 else z_next, part, k_recv.at[2] if part else x_recv.at[t])
            push(t, sib, part, k_recv.at[3] if part else x_recv.at[t])

    def gather_far(part):
        if part:
            arrived(xb.at[pl.ds(0, 2), ks], k_recv.at[2], z_next)
        for t in distant:
            if not part:
                here(t)
            push(t, sib, part, k_recv.at[4] if part else x_recv.at[t])

    def source(k):
        return 1 - c if k % 2 == 0 else c, lax.rem(z + OFFSETS[k // 2], NZ)

    xn1, xp1, xf = lax.rem(x + 1, NX), lax.rem(x + 3, NX), lax.rem(x + 2, NX)

    def matmul(k):
        hs, zz = source(k)
        here(t_of(hs, zz, 1 - c))
        gain = gain_ref[...].astype(F32).reshape(1, DS)
        for g in range(8):
            for i in range(2):
                v = xb[t_of(hs, zz, i), g].astype(F32) * gain
                xn[pl.ds(g * 16 + i * 8, 8), :] = v
        lhs = xn[...].astype(BF16)
        if k == 0:
            loads[0].wait()
        acc = jnp.dot(lhs, wu[...], preferred_element_type=F32)
        for g in range(8):
            for i in range(2):
                lo = g * 16 + i * 8
                pu[k, g % 2, g // 2, i] = acc[lo : lo + 8].astype(BF16)
        send(pu.at[k, 1 - y], u_y.at[k], u_send, u_done.at[k, 0], y_other)
        if k == 0:
            loads[1].wait()
        acc = jnp.dot(lhs, wg[...], preferred_element_type=F32).astype(BF16)
        for g in range(8):
            pg[k, g // 2, g % 2] = acc[g * 16 : g * 16 + 16]
        send(pg.at[k, xf, 0], g_relay.at[k, 0], g_send, g_done.at[k, 0], x_next)
        send(pg.at[k, xf, 1], g_relay.at[k, 1], g_send, g_done.at[k, 0], x_prev)
        send(pg.at[k, xn1, 1], g_recv.at[k, 0, 1], g_send, g_done.at[k, 1], x_next)
        send(pg.at[k, xp1, 0], g_recv.at[k, 1, 0], g_send, g_done.at[k, 1], x_prev)

    def gate_relay(k):
        arrived(g_relay.at[k], g_done.at[k, 0], x_next)
        v = pg[k, xn1, 0].astype(F32) + g_relay[k, 0].astype(F32)
        pg[k, xn1, 0] = v.astype(BF16)
        send(pg.at[k, xn1, 0], g_recv.at[k, 0, 0], g_send, g_done.at[k, 1], x_next)
        v = pg[k, xp1, 1].astype(F32) + g_relay[k, 1].astype(F32)
        pg[k, xp1, 1] = v.astype(BF16)
        send(pg.at[k, xp1, 1], g_recv.at[k, 1, 1], g_send, g_done.at[k, 1], x_prev)

    def gate_over_x(k, yy):
        return (
            pg[k, x, yy].astype(F32) + g_recv[k, 0, yy].astype(F32) + g_recv[k, 1, yy].astype(F32)
        )

    def gate_y(k):
        arrived(g_recv.at[k], g_done.at[k, 1], x_next)
        ysend[k] = gate_over_x(k, 1 - y).astype(BF16)
        send(ysend.at[k], yrecv.at[k], g_send, g_done.at[k, 2], y_other)

    def up_over_y(k):
        arrived(u_y.at[k], u_done.at[k, 0], y_other)
        for xx in (xf, xn1, xp1, x):
            v = pu[k, y, xx].astype(F32) + u_y[k, xx].astype(F32)
            pu[k, y, xx] = v.astype(BF16)
            if xx is xf:
                send(pu.at[k, y, xf, 0], u_relay.at[k, 0], u_send, u_done.at[k, 1], x_next)
                send(pu.at[k, y, xf, 1], u_relay.at[k, 1], u_send, u_done.at[k, 1], x_prev)
            if xx is xn1:
                send(
                    pu.at[k, y, xx, 1], u_recv.at[k, 0, 1], u_send, u_done.at[k, 2], x_next
                )
            if xx is xp1:
                send(
                    pu.at[k, y, xx, 0], u_recv.at[k, 1, 0], u_send, u_done.at[k, 2], x_prev
                )

    def up_relay(k):
        arrived(u_relay.at[k], u_done.at[k, 1], x_next)
        v = pu[k, y, xn1, 0].astype(F32) + u_relay[k, 0].astype(F32)
        pu[k, y, xn1, 0] = v.astype(BF16)
        send(pu.at[k, y, xn1, 0], u_recv.at[k, 0, 0], u_send, u_done.at[k, 2], x_next)
        v = pu[k, y, xp1, 1].astype(F32) + u_relay[k, 1].astype(F32)
        pu[k, y, xp1, 1] = v.astype(BF16)
        send(pu.at[k, y, xp1, 1], u_recv.at[k, 1, 1], u_send, u_done.at[k, 2], x_prev)

    def hidden(k):
        hs, zz = source(k)
        if k in (0, 2, 6):
            blocks, i = {0: (2, 0), 2: (4, 3), 6: (2, 4)}[k]
            arrived(xb.at[pl.ds(0, blocks), ks], k_recv.at[i], sib)
        lanes = pl.ds(pl.multiple_of(lax.rem(tp, 8) * 128, 128), 128)
        slots = [xb[t_of(hs, zz, i), 8 + lax.div(tp, 8), :, lanes].astype(F32) for i in range(2)]
        slots = jnp.concatenate(slots, axis=0)
        lane = lax.broadcasted_iota(jnp.int32, (16, 128), 1)
        inv = jnp.sum(
            jnp.where((lane >= 112) & (lane < 115), slots, 0.0), axis=1, keepdims=True
        )
        byte = jnp.dot(slots.astype(BF16), spread[...], preferred_element_type=F32)
        unit = lax.broadcasted_iota(jnp.int32, (16, FU), 1)
        bit = (byte.astype(jnp.int32) >> (unit & 7)) & 1
        keep = 2.0 * bit.astype(F32)
        arrived(yrecv.at[k], g_done.at[k, 2], y_other)
        gate = (gate_over_x(k, y) + yrecv[k].astype(F32)) * inv
        arrived(u_recv.at[k], u_done.at[k, 2], x_next)
        up = pu[k, y, x].astype(F32) + u_recv[k, 0].astype(F32) + u_recv[k, 1].astype(F32)
        up = up.reshape(16, FU) * inv
        hid[k, x, y] = (gate / (1.0 + jnp.exp(-gate)) * up * keep).astype(BF16)
        near_y, far_y = 1 + y, 2 - y
        block = hid.at[k, x, y]
        send(block, block, h_send, h_done.at[k, 0], y_other)
        send(block, block, h_send, h_done.at[k, near_y], x_next)
        send(block, block, h_send, h_done.at[k, far_y], x_prev)

    def pass_y(k):
        block = hid.at[k, x, 1 - y]
        arrived(block, h_done.at[k, 0], y_other)
        near_y, far_y = 1 + y, 2 - y
        send(block, block, h_send, h_done.at[k, far_y], x_next)
        send(block, block, h_send, h_done.at[k, near_y], x_prev)

    def pass_x(k):
        arrived(hid.at[k, 0], h_done.at[k, 1], x_next)
        block = hid.at[k, xp1, 0]
        send(block, block, h_send, h_done.at[k, 2], x_next)
        block = hid.at[k, xn1, 1]
        send(block, block, h_send, h_done.at[k, 2], x_prev)

    def down(k):
        arrived(hid.at[k, pl.ds(0, 2)], h_done.at[k, 2], x_next)
        if k == 0:
            loads[2].wait()
        acc = jnp.dot(hid[k].reshape(128, FU), wd[...], preferred_element_type=F32)
        i = k // 2
        if k % 2 == 0:
            osum[i] = acc.astype(BF16).reshape(8, 16, DS)
            send(osum.at[i], orecv.at[i], o_send, o_recv.at[i], sib)
            return
        _, zz = source(k)
        arrived(orecv.at[i], o_recv.at[i], sib)
        fsend[i] = (acc.reshape(8, 16, DS) + orecv[i].astype(F32)).astype(BF16)
        for dh, dz in tp_others:
            send(
                fsend.at[i, lax.rem(z + dz, NZ) * NY + lax.rem(h + dh, NH)],
                frecv.at[h * NZ + z, zz],
                f_send,
                f_recv,
                dev_t(dh, dz),
            )

    matmul(0)
    matmul(1)
    gate_relay(0)
    up_over_y(0)
    gate_relay(1)
    gather_near(0)
    gate_y(0)
    up_relay(0)
    up_over_y(1)
    matmul(2)
    matmul(3)
    gate_y(1)
    up_relay(1)
    matmul(4)
    hidden(0)
    up_over_y(2)
    matmul(5)
    gate_relay(2)
    gate_relay(3)
    gather_near(1)
    up_relay(2)
    gate_relay(5)
    gate_relay(4)
    up_over_y(3)
    gather_far(0)
    up_over_y(4)
    gate_y(2)
    pass_y(0)
    hidden(1)
    matmul(6)
    up_relay(3)
    up_over_y(5)
    gate_y(4)
    pass_x(0)
    gate_y(3)
    pass_y(1)
    up_relay(4)
    gate_y(5)
    hidden(2)
    gate_relay(6)
    up_relay(5)
    gather_far(1)
    matmul(7)
    down(0)
    pass_x(1)
    up_over_y(6)
    hidden(3)
    gate_relay(7)
    pass_y(2)
    hidden(4)
    hidden(5)
    up_over_y(7)
    pass_y(3)
    gate_y(6)
    up_relay(6)
    down(1)
    gate_y(7)
    pass_x(2)
    pass_y(4)
    up_relay(7)
    pass_x(3)
    pass_y(5)
    hidden(6)
    down(2)
    pass_x(4)
    hidden(7)
    down(3)
    pass_y(6)
    pass_x(5)
    pass_y(7)
    down(4)
    pass_x(6)
    down(5)
    pass_x(7)
    down(6)
    down(7)

    left(xb.at[tp, pl.ds(0, 7)], a_send.at[0], y_other)
    left(xb.at[tp, pl.ds(0, 8)], a_send.at[1], h_other)
    left(xb.at[tp, ks], k_sem.at[0], h_other)
    left(xb.at[pl.ds(0, 14), xs], x_send.at[0], sib)
    left(xb.at[pl.ds(0, 14), ks], x_send.at[1], sib)
    left(pg.at[pl.ds(0, 7)], g_send, x_next)
    left(pu.at[pl.ds(0, 7)], u_send, x_next)
    left(hid.at[pl.ds(0, 7)], h_send, x_next)
    left(osum, o_send, sib)
    arrived(frecv.at[pl.ds(0, 7)], f_recv, h_other)
    for k in range(4):
        zz = lax.rem(z + OFFSETS[k], NZ)
        total = fsend[k, z * NY + h].astype(F32)
        res = jnp.concatenate(
            [xb[t_of(c, zz, b), z * NY + h].astype(F32) for b in range(2)], axis=0
        )
        total = total + res
        for dh, dz in tp_others:
            src = lax.rem(h + dh, NH) * NZ + lax.rem(z + dz, NZ)
            total = total + frecv[src, zz].astype(F32)
        rounded = total.astype(BF16)
        rows = pl.ds(pl.multiple_of(zz * 16, 16), 16)
        obuf[rows, :] = rounded
        wide = rounded.astype(F32)
        wide = wide * wide
        folded = wide[:, 0:128]
        for i in range(1, 8):
            folded = folded + wide[:, i * 128 : (i + 1) * 128]
        sq[rows, :] = folded
    result = pltpu.make_async_copy(obuf, out_ref, l_sem.at[0])
    result.start()
    rowsum = jnp.sum(sq[...].T, axis=0, keepdims=True)
    csend[:, 0:64] = jnp.broadcast_to(rowsum, (8, 64))
    csend[:, 64:128] = jnp.zeros((8, 64), F32)
    for dx, dy in dp_others:
        send(csend, crecv.at[mine], c_send, c_recv, dev_d(dx, dy))
    left(frecv.at[pl.ds(0, 7)], f_send, h_other)
    total = csend[...]
    arrived(crecv.at[pl.ds(0, 7)], c_recv, y_other)
    for dx, dy in dp_others:
        g = lax.rem(x + dx, NX) * NY + lax.rem(y + dy, NY)
        total = total + crecv[g]
    rc_ref[...] = total[0, 0:64] / D
    result.wait()
    left(crecv.at[pl.ds(0, 7)], c_send, y_other)


def on_device(saved_input, keep_bits, norm_gain, gate_weight, up_weight, down_weight):
    vmem = pl.BlockSpec(memory_space=pltpu.VMEM)
    hbm = pl.BlockSpec(memory_space=pltpu.HBM)
    dma = pltpu.SemaphoreType.DMA
    out, check = pl.pallas_call(
        kernel,
        out_shape=(
            jax.ShapeDtypeStruct((64, DS), BF16),
            jax.ShapeDtypeStruct((64,), F32),
        ),
        in_specs=[hbm] * 6,
        out_specs=(hbm, vmem),
        scratch_shapes=[
            pltpu.VMEM((DS, FU), BF16),
            pltpu.VMEM((DS, FU), BF16),
            pltpu.VMEM((FU, DS), BF16),
            pltpu.VMEM((128, FU), BF16),
            pltpu.VMEM((8, 512), jnp.int32),
            pltpu.VMEM((8, 448), jnp.int32),
            pltpu.VMEM((DS,), BF16),
            pltpu.VMEM((8, D), BF16),
            pltpu.VMEM((16, 10, 8, DS), BF16),
            pltpu.VMEM((128, DS), F32),
            pltpu.VMEM((8, 4, 2, 16, FU), BF16),
            pltpu.VMEM((8, 2, 4, 2, 8, FU), BF16),
            pltpu.VMEM((8, 2, 16, FU), BF16),
            pltpu.VMEM((8, 2, 2, 16, FU), BF16),
            pltpu.VMEM((8, 2, 8, FU), BF16),
            pltpu.VMEM((8, 2, 2, 8, FU), BF16),
            pltpu.VMEM((8, 4, 2, 8, FU), BF16),
            pltpu.VMEM((8, 16, FU), BF16),
            pltpu.VMEM((8, 16, FU), BF16),
            pltpu.VMEM((8, 4, 2, 16, FU), BF16),
            pltpu.VMEM((4, 8, 16, DS), BF16),
            pltpu.VMEM((4, 8, 16, DS), BF16),
            pltpu.VMEM((4, 8, 16, DS), BF16),
            pltpu.VMEM((8, 4, 16, DS), BF16),
            pltpu.VMEM((64, DS), BF16),
            pltpu.VMEM((64, 128), F32),
            pltpu.VMEM((8, 128), F32),
            pltpu.VMEM((8, 8, 128), F32),
            dma((3,)),
            dma((4,)),
            dma((2,)),
            dma((2,)),
            dma((2,)),
            dma((2,)),
            dma((16,)),
            dma((5,)),
            dma,
            dma((8, 3)),
            dma,
            dma((8, 3)),
            dma,
            dma((8, 3)),
            dma,
            dma((4,)),
            dma,
            dma,
            dma,
            dma,
        ],
        compiler_params=pltpu.CompilerParams(
            collective_id=0, has_side_effects=True, vmem_limit_bytes=56 * 1024 * 1024
        ),
        name="block",
    )(saved_input, keep_bits, norm_gain, gate_weight, up_weight, down_weight)
    return out, check


def solution(mesh):
    both = ("dp", "tensor")
    return jax.shard_map(
        on_device,
        mesh=mesh,
        in_specs=(
            P(both, None),
            P(both, None),
            P("dp"),
            P("dp", "tensor"),
            P("dp", "tensor"),
            P("tensor", "dp"),
        ),
        out_specs=(P("tensor", "dp"), P("tensor")),
        check_vma=False,
    )
```

```python
import jax
import jax.numpy as jnp
from jax import lax
from jax.experimental import pallas as pl
from jax.experimental.pallas import tpu as pltpu
from jax.sharding import PartitionSpec as P

D = 8192
DS = 1024
FU = 896
FA, FB = 1024, 768
MESH = pl.DeviceIdType.MESH
F32 = jnp.float32
BF16 = jnp.bfloat16
NX, NY, NH, NZ = 4, 2, 2, 4
OFFSETS = (0, 1, 3, 2)


def kernel(
    x_hbm,
    kb_hbm,
    gain_hbm,
    wg_hbm,
    wu_hbm,
    wd_hbm,
    out_ref,
    rc_ref,
    wg,
    wu,
    wd,
    spread,
    words,
    kb_ref,
    gain_ref,
    x_ref,
    xb,
    xn,
    pg,
    pu,
    g_relay,
    g_recv,
    u_relay,
    u_recv,
    u_y,
    ysend,
    yrecv,
    hid,
    osum,
    orecv,
    fsend,
    frecv,
    obuf,
    sq,
    csend,
    crecv,
    w_sem,
    l_sem,
    a_send,
    a_recv,
    k_sem,
    x_send,
    x_recv,
    k_recv,
    g_send,
    g_done,
    u_send,
    u_done,
    h_send,
    h_done,
    o_send,
    o_recv,
    f_send,
    f_recv,
    c_send,
    c_recv,
):
    dp = lax.axis_index("dp")
    tp = lax.axis_index("tensor")
    x, y = lax.rem(dp, NX), lax.div(dp, NX)
    c, z, h = lax.rem(tp, 2), lax.rem(lax.div(tp, 2), NZ), lax.div(tp, 2 * NZ)

    def t_of(hh, zz, cc):
        return (hh * NZ + zz) * 2 + cc

    def dev_d(dx, dy, dh=0):
        d = lax.rem(y + dy, NY) * NX + lax.rem(x + dx, NX)
        return {"dp": d, "tensor": t_of(lax.rem(h + dh, NH), z, c)}

    def dev_t(dh, dz, dc=0):
        t = t_of(lax.rem(h + dh, NH), lax.rem(z + dz, NZ), lax.rem(c + dc, 2))
        return {"dp": dp, "tensor": t}

    x_next, x_prev = dev_d(1, 0), dev_d(NX - 1, 0)
    y_other = dev_d(0, 1)
    sib = dev_t(0, 0, 1)
    h_other = dev_t(1, 0)
    z_next, z_prev = dev_t(0, 1), dev_t(0, NZ - 1)

    def send(src, dst, ssem, rsem, device):
        copy = pltpu.make_async_remote_copy(
            src_ref=src,
            dst_ref=dst,
            send_sem=ssem,
            recv_sem=rsem,
            device_id=device,
            device_id_type=MESH,
        )
        copy.start()

    def arrived(dst, rsem, device):
        pltpu.make_async_remote_copy(
            src_ref=dst,
            dst_ref=dst,
            send_sem=rsem,
            recv_sem=rsem,
            device_id=device,
            device_id_type=MESH,
        ).wait_recv()

    def left(src, ssem, device):
        pltpu.make_async_remote_copy(
            src_ref=src,
            dst_ref=src,
            send_sem=ssem,
            recv_sem=ssem,
            device_id=device,
            device_id_type=MESH,
        ).wait_send()

    dp_others = [(dx, dy) for dx in (1, 3, 2, 0) for dy in (0, 1) if (dx, dy) != (0, 0)]
    tp_others = [(dh, dz) for dz in (2, 1, 3, 0) for dh in (1, 0) if (dh, dz) != (0, 0)]

    row_others = [(dx, dy, 0) for dx, dy in dp_others]
    row_others += [(dx, dy, 1) for dx, dy in [*dp_others, (0, 0)]]

    loads = [
        pltpu.make_async_copy(wu_hbm.at[:, pl.ds(FA - FU, FB)], wu, w_sem.at[0]),
        pltpu.make_async_copy(wg_hbm, wg.at[:, pl.ds(0, FU)], w_sem.at[1]),
        pltpu.make_async_copy(wd_hbm, wd, w_sem.at[2]),
        pltpu.make_async_copy(
            wu_hbm.at[:, pl.ds(0, FA - FU)], wg.at[:, pl.ds(FU, FA - FU)], w_sem.at[3]
        ),
    ]
    rows_in = [
        pltpu.make_async_copy(x_hbm, x_ref, l_sem.at[0]),
        pltpu.make_async_copy(kb_hbm, kb_ref, l_sem.at[2]),
        pltpu.make_async_copy(gain_hbm, gain_ref, l_sem.at[3]),
    ]
    for load in rows_in:
        load.start()
    mine = x * NY + y

    barrier = pltpu.get_barrier_semaphore()
    for dx, dy, dh in row_others:
        pl.semaphore_signal(barrier, inc=1, device_id=dev_d(dx, dy, dh), device_id_type=MESH)
    for dh, dz in tp_others:
        if dz == 0:
            continue
        pl.semaphore_signal(barrier, inc=1, device_id=dev_t(dh, dz), device_id_type=MESH)
    pl.semaphore_signal(barrier, inc=1, device_id=sib, device_id_type=MESH)
    for load in rows_in:
        load.wait()
    own = pltpu.make_async_copy(
        x_ref.at[:, pl.ds(pl.multiple_of(dp * DS, DS), DS)], xb.at[tp, mine], l_sem.at[1]
    )
    own.start()
    wide = x_ref[...].astype(F32)
    inv = lax.rsqrt(jnp.sum(wide * wide, axis=1, keepdims=True) / D + 1e-05)
    hi = inv.astype(BF16).astype(F32)
    mid = (inv - hi).astype(BF16).astype(F32)
    low = inv - hi - mid
    words[...] = jnp.zeros((8, 512), jnp.int32)
    words[:, 0:448] = kb_ref[...]
    lane = lax.broadcasted_iota(jnp.int32, (8, 128), 1)
    scale = jnp.where(lane == 112, hi, jnp.where(lane == 113, mid, low))
    scale = jnp.where((lane >= 112) & (lane < 115), scale, 0.0)
    for t in range(16):
        tile, start = divmod(28 * t, 128)
        piece = words[:, tile * 128 : tile * 128 + 128]
        if start:
            piece = pltpu.roll(piece, 128 - start, 1)
        if start + 28 > 128:
            after = pltpu.roll(words[:, tile * 128 + 128 : tile * 128 + 256], 128 - start, 1)
            piece = jnp.where(lane < 128 - start, piece, after)
        taken = jnp.zeros((8, 128), jnp.int32)
        for j in range(4):
            byte = (piece >> (8 * j)) & 255
            if j:
                byte = pltpu.roll(byte, 28 * j, 1)
            taken = jnp.where((lane >= 28 * j) & (lane < 28 * j + 28), byte, taken)
        slot = (taken.astype(F32) + scale).astype(BF16)
        xb[tp, 8 + t // 8, :, (t % 8) * 128 : (t % 8) * 128 + 128] = slot
    pl.semaphore_wait(barrier, len(row_others) + 7)

    for dx, dy, dh in row_others:
        there = lax.rem(y + dy, NY) * NX + lax.rem(x + dx, NX)
        send(
            x_ref.at[:, pl.ds(pl.multiple_of(there * DS, DS), DS)],
            xb.at[tp, mine],
            a_send.at[dh],
            a_recv.at[dh],
            dev_d(dx, dy, dh),
        )
    send(xb.at[tp, pl.ds(8, 2)], xb.at[tp, pl.ds(8, 2)], k_sem.at[0], k_sem.at[1], h_other)
    for load in loads:
        load.start()
    row = lax.broadcasted_iota(jnp.int32, (128, FU), 0)
    col = lax.broadcasted_iota(jnp.int32, (128, FU), 1)
    place = ((col & 31) >> 3) * 28 + (col >> 5)
    spread[...] = jnp.where(row == place, 1.0, 0.0).astype(BF16)
    xs, ks = pl.ds(0, 8), pl.ds(8, 2)

    def push(t, device, part, rsem):
        cells = xb.at[t, ks if part else xs]
        send(cells, cells, x_send.at[part], rsem, device)

    def here(t):
        arrived(xb.at[t, xs], x_recv.at[t], sib)

    def push_x(t, *devices):
        for device in devices:
            push(t, device, 0, x_recv.at[t])

    z1, z3, z2 = lax.rem(z + 1, NZ), lax.rem(z + 3, NZ), lax.rem(z + 2, NZ)
    hh = 1 - h
    across = t_of(hh, z, c)
    own.wait()
    for there in range(2):
        if there == 0:
            arrived(xb.at[tp, pl.ds(0, 7)], a_recv.at[0], y_other)
        else:
            arrived(xb.at[across, pl.ds(0, 8)], a_recv.at[1], h_other)
        push_x(across if there else tp, sib, z_next, z_prev)
    for t in (tp, across):
        if t is across:
            arrived(xb.at[across, ks], k_sem.at[1], h_other)
        push(t, sib, 1, k_recv.at[0])
        push(t, z_next, 1, k_recv.at[1])
        push(t, z_prev, 1, k_recv.at[1])

    near = [t_of(h, z1, c), t_of(h, z3, c), t_of(hh, z3, c), t_of(hh, z1, c)]
    distant = [t_of(h, z2, c), t_of(hh, z2, c)]

    def gather_near(part):
        if part:
            arrived(xb.at[pl.ds(0, 4), ks], k_recv.at[1], z_next)
        for i, t in enumerate(near):
            if not part:
                here(t)
            if i in (0, 2):
                push(t, z_prev if i == 0 else z_next, part, k_recv.at[2] if part else x_recv.at[t])
            push(t, sib, part, k_recv.at[3] if part else x_recv.at[t])

    def gather_far(part):
        if part:
            arrived(xb.at[pl.ds(0, 2), ks], k_recv.at[2], z_next)
        for t in distant:
            if not part:
                here(t)
            push(t, sib, part, k_recv.at[4] if part else x_recv.at[t])

    def source(k):
        return 1 - c if k % 2 == 0 else c, lax.rem(z + OFFSETS[k // 2], NZ)

    xn1, xp1, xf = lax.rem(x + 1, NX), lax.rem(x + 3, NX), lax.rem(x + 2, NX)

    def matmul(k):
        hs, zz = source(k)
        here(t_of(hs, zz, 1 - c))
        gain = gain_ref[...].astype(F32).reshape(1, DS)
        for g in range(8):
            for i in range(2):
                v = xb[t_of(hs, zz, i), g].astype(F32) * gain
                xn[pl.ds(g * 16 + i * 8, 8), :] = v
        lhs = xn[...].astype(BF16)
        if k == 0:
            loads[0].wait()
        acc = jnp.dot(lhs, wu[...], preferred_element_type=F32)
        for g in range(8):
            for i in range(2):
                lo = g * 16 + i * 8
                pu[k, g % 2, g // 2, i] = acc[lo : lo + 8].astype(BF16)
        send(pu.at[k, 1 - y], u_y.at[k], u_send, u_done.at[k, 0], y_other)
        if k == 0:
            loads[1].wait()
            loads[3].wait()
        acc = jnp.dot(lhs, wg[...], preferred_element_type=F32).astype(BF16)
        for g in range(8):
            pg[k, g // 2, g % 2] = acc[g * 16 : g * 16 + 16]
        send(pg.at[k, xf, 0], g_relay.at[k, 0], g_send, g_done.at[k, 0], x_next)
        send(pg.at[k, xf, 1], g_relay.at[k, 1], g_send, g_done.at[k, 0], x_prev)
        send(pg.at[k, xn1, 1], g_recv.at[k, 0, 1], g_send, g_done.at[k, 1], x_next)
        send(pg.at[k, xp1, 0], g_recv.at[k, 1, 0], g_send, g_done.at[k, 1], x_prev)

    def gate_relay(k):
        arrived(g_relay.at[k], g_done.at[k, 0], x_next)
        v = pg[k, xn1, 0].astype(F32) + g_relay[k, 0].astype(F32)
        pg[k, xn1, 0] = v.astype(BF16)
        send(pg.at[k, xn1, 0], g_recv.at[k, 0, 0], g_send, g_done.at[k, 1], x_next)
        v = pg[k, xp1, 1].astype(F32) + g_relay[k, 1].astype(F32)
        pg[k, xp1, 1] = v.astype(BF16)
        send(pg.at[k, xp1, 1], g_recv.at[k, 1, 1], g_send, g_done.at[k, 1], x_prev)

    def gate_over_x(k, yy):
        return (
            pg[k, x, yy].astype(F32) + g_recv[k, 0, yy].astype(F32) + g_recv[k, 1, yy].astype(F32)
        )

    def gate_y(k):
        arrived(g_recv.at[k], g_done.at[k, 1], x_next)
        ysend[k] = gate_over_x(k, 1 - y).astype(BF16)
        send(ysend.at[k], yrecv.at[k], g_send, g_done.at[k, 2], y_other)

    def up_over_y(k):
        arrived(u_y.at[k], u_done.at[k, 0], y_other)
        for xx in (xf, xn1, xp1, x):
            v = pu[k, y, xx].astype(F32) + u_y[k, xx].astype(F32)
            pu[k, y, xx] = v.astype(BF16)
            if xx is xf:
                send(pu.at[k, y, xf, 0], u_relay.at[k, 0], u_send, u_done.at[k, 1], x_next)
                send(pu.at[k, y, xf, 1], u_relay.at[k, 1], u_send, u_done.at[k, 1], x_prev)
            if xx is xn1:
                send(
                    pu.at[k, y, xx, 1], u_recv.at[k, 0, 1], u_send, u_done.at[k, 2], x_next
                )
            if xx is xp1:
                send(
                    pu.at[k, y, xx, 0], u_recv.at[k, 1, 0], u_send, u_done.at[k, 2], x_prev
                )

    def up_relay(k):
        arrived(u_relay.at[k], u_done.at[k, 1], x_next)
        v = pu[k, y, xn1, 0].astype(F32) + u_relay[k, 0].astype(F32)
        pu[k, y, xn1, 0] = v.astype(BF16)
        send(pu.at[k, y, xn1, 0], u_recv.at[k, 0, 0], u_send, u_done.at[k, 2], x_next)
        v = pu[k, y, xp1, 1].astype(F32) + u_relay[k, 1].astype(F32)
        pu[k, y, xp1, 1] = v.astype(BF16)
        send(pu.at[k, y, xp1, 1], u_recv.at[k, 1, 1], u_send, u_done.at[k, 2], x_prev)

    def hidden(k):
        hs, zz = source(k)
        if k in (0, 2, 6):
            blocks, i = {0: (2, 0), 2: (4, 3), 6: (2, 4)}[k]
            arrived(xb.at[pl.ds(0, blocks), ks], k_recv.at[i], sib)
        lanes = pl.ds(pl.multiple_of(lax.rem(tp, 8) * 128, 128), 128)
        slots = [xb[t_of(hs, zz, i), 8 + lax.div(tp, 8), :, lanes].astype(F32) for i in range(2)]
        slots = jnp.concatenate(slots, axis=0)
        lane = lax.broadcasted_iota(jnp.int32, (16, 128), 1)
        inv = jnp.sum(
            jnp.where((lane >= 112) & (lane < 115), slots, 0.0), axis=1, keepdims=True
        )
        byte = jnp.dot(slots.astype(BF16), spread[...], preferred_element_type=F32)
        unit = lax.broadcasted_iota(jnp.int32, (16, FU), 1)
        bit = (byte.astype(jnp.int32) >> (unit & 7)) & 1
        keep = 2.0 * bit.astype(F32)
        arrived(yrecv.at[k], g_done.at[k, 2], y_other)
        first = gate_over_x(k, y) + yrecv[k].astype(F32)
        gate = first[:, :FU] * inv
        arrived(u_recv.at[k], u_done.at[k, 2], x_next)
        up = pu[k, y, x].astype(F32) + u_recv[k, 0].astype(F32) + u_recv[k, 1].astype(F32)
        up = jnp.concatenate((first[:, FU:], up.reshape(16, FB)), axis=1) * inv
        hid[k, x, y] = (gate / (1.0 + jnp.exp(-gate)) * up * keep).astype(BF16)
        near_y, far_y = 1 + y, 2 - y
        block = hid.at[k, x, y]
        send(block, block, h_send, h_done.at[k, 0], y_other)
        send(block, block, h_send, h_done.at[k, near_y], x_next)
        send(block, block, h_send, h_done.at[k, far_y], x_prev)

    def pass_y(k):
        block = hid.at[k, x, 1 - y]
        arrived(block, h_done.at[k, 0], y_other)
        near_y, far_y = 1 + y, 2 - y
        send(block, block, h_send, h_done.at[k, far_y], x_next)
        send(block, block, h_send, h_done.at[k, near_y], x_prev)

    def pass_x(k):
        arrived(hid.at[k, 0], h_done.at[k, 1], x_next)
        block = hid.at[k, xp1, 0]
        send(block, block, h_send, h_done.at[k, 2], x_next)
        block = hid.at[k, xn1, 1]
        send(block, block, h_send, h_done.at[k, 2], x_prev)

    def down(k):
        arrived(hid.at[k, pl.ds(0, 2)], h_done.at[k, 2], x_next)
        if k == 0:
            loads[2].wait()
        acc = jnp.dot(hid[k].reshape(128, FU), wd[...], preferred_element_type=F32)
        i = k // 2
        if k % 2 == 0:
            osum[i] = acc.astype(BF16).reshape(8, 16, DS)
            send(osum.at[i], orecv.at[i], o_send, o_recv.at[i], sib)
            return
        _, zz = source(k)
        arrived(orecv.at[i], o_recv.at[i], sib)
        fsend[i] = (acc.reshape(8, 16, DS) + orecv[i].astype(F32)).astype(BF16)
        for dh, dz in tp_others:
            send(
                fsend.at[i, lax.rem(z + dz, NZ) * NY + lax.rem(h + dh, NH)],
                frecv.at[h * NZ + z, zz],
                f_send,
                f_recv,
                dev_t(dh, dz),
            )

    matmul(0)
    matmul(1)
    gate_relay(0)
    up_over_y(0)
    gate_relay(1)
    gather_near(0)
    gate_y(0)
    up_relay(0)
    up_over_y(1)
    matmul(2)
    matmul(3)
    gate_y(1)
    up_relay(1)
    matmul(4)
    hidden(0)
    up_over_y(2)
    matmul(5)
    gate_relay(2)
    gate_relay(3)
    gather_near(1)
    up_relay(2)
    gate_relay(5)
    gate_relay(4)
    up_over_y(3)
    gather_far(0)
    up_over_y(4)
    gate_y(2)
    pass_y(0)
    hidden(1)
    matmul(6)
    up_relay(3)
    up_over_y(5)
    gate_y(4)
    pass_x(0)
    gate_y(3)
    pass_y(1)
    up_relay(4)
    gate_y(5)
    hidden(2)
    gate_relay(6)
    up_relay(5)
    gather_far(1)
    matmul(7)
    down(0)
    pass_x(1)
    up_over_y(6)
    hidden(3)
    gate_relay(7)
    pass_y(2)
    hidden(4)
    hidden(5)
    up_over_y(7)
    pass_y(3)
    gate_y(6)
    up_relay(6)
    down(1)
    gate_y(7)
    pass_x(2)
    pass_y(4)
    up_relay(7)
    pass_x(3)
    pass_y(5)
    hidden(6)
    down(2)
    pass_x(4)
    hidden(7)
    down(3)
    pass_y(6)
    pass_x(5)
    pass_y(7)
    down(4)
    pass_x(6)
    down(5)
    pass_x(7)
    down(6)
    down(7)

    left(xb.at[tp, pl.ds(0, 7)], a_send.at[0], y_other)
    left(xb.at[tp, pl.ds(0, 8)], a_send.at[1], h_other)
    left(xb.at[tp, ks], k_sem.at[0], h_other)
    left(xb.at[pl.ds(0, 14), xs], x_send.at[0], sib)
    left(xb.at[pl.ds(0, 14), ks], x_send.at[1], sib)
    left(pg.at[pl.ds(0, 7)], g_send, x_next)
    left(pu.at[pl.ds(0, 7)], u_send, x_next)
    left(hid.at[pl.ds(0, 7)], h_send, x_next)
    left(osum, o_send, sib)
    arrived(frecv.at[pl.ds(0, 7)], f_recv, h_other)
    for k in range(4):
        zz = lax.rem(z + OFFSETS[k], NZ)
        total = fsend[k, z * NY + h].astype(F32)
        res = jnp.concatenate(
            [xb[t_of(c, zz, b), z * NY + h].astype(F32) for b in range(2)], axis=0
        )
        total = total + res
        for dh, dz in tp_others:
            src = lax.rem(h + dh, NH) * NZ + lax.rem(z + dz, NZ)
            total = total + frecv[src, zz].astype(F32)
        rounded = total.astype(BF16)
        rows = pl.ds(pl.multiple_of(zz * 16, 16), 16)
        obuf[rows, :] = rounded
        wide = rounded.astype(F32)
        wide = wide * wide
        folded = wide[:, 0:128]
        for i in range(1, 8):
            folded = folded + wide[:, i * 128 : (i + 1) * 128]
        sq[rows, :] = folded
    result = pltpu.make_async_copy(obuf, out_ref, l_sem.at[0])
    result.start()
    rowsum = jnp.sum(sq[...].T, axis=0, keepdims=True)
    csend[:, 0:64] = jnp.broadcast_to(rowsum, (8, 64))
    csend[:, 64:128] = jnp.zeros((8, 64), F32)
    for dx, dy in dp_others:
        send(csend, crecv.at[mine], c_send, c_recv, dev_d(dx, dy))
    left(frecv.at[pl.ds(0, 7)], f_send, h_other)
    total = csend[...]
    arrived(crecv.at[pl.ds(0, 7)], c_recv, y_other)
    for dx, dy in dp_others:
        g = lax.rem(x + dx, NX) * NY + lax.rem(y + dy, NY)
        total = total + crecv[g]
    rc_ref[...] = total[0, 0:64] / D
    result.wait()
    left(crecv.at[pl.ds(0, 7)], c_send, y_other)


def finish(out_ref, check_ref, out_hbm, check_hbm, rows, check, sems):
    def copies(into):
        j = 0 if into else 1
        moves = []
        for i in range(4):
            held, cells = rows.at[i], pl.ds(i * 16, 16)
            src, dst = (out_ref.at[cells], held) if into else (held, out_hbm.at[cells])
            moves.append(pltpu.make_async_copy(src, dst, sems.at[j, i]))
        src, dst = (check_ref, check) if into else (check, check_hbm)
        moves.append(pltpu.make_async_copy(src, dst, sems.at[j, 4]))
        return moves

    taken, put = copies(True), copies(False)
    for move in taken:
        move.start()
    for first, second in zip(taken, put):
        first.wait()
        second.start()
    for move in put:
        move.wait()


def on_device(saved_input, keep_bits, norm_gain, gate_weight, up_weight, down_weight):
    vmem = pl.BlockSpec(memory_space=pltpu.VMEM)
    hbm = pl.BlockSpec(memory_space=pltpu.HBM)
    dma = pltpu.SemaphoreType.DMA
    out, check = pl.pallas_call(
        kernel,
        out_shape=(
            jax.ShapeDtypeStruct((64, DS), BF16),
            jax.ShapeDtypeStruct((64,), F32),
        ),
        in_specs=[hbm] * 6,
        out_specs=(hbm, vmem),
        scratch_shapes=[
            pltpu.VMEM((DS, FA), BF16),
            pltpu.VMEM((DS, FB), BF16),
            pltpu.VMEM((FU, DS), BF16),
            pltpu.VMEM((128, FU), BF16),
            pltpu.VMEM((8, 512), jnp.int32),
            pltpu.VMEM((8, 448), jnp.int32),
            pltpu.VMEM((DS,), BF16),
            pltpu.VMEM((8, D), BF16),
            pltpu.VMEM((16, 10, 8, DS), BF16),
            pltpu.VMEM((128, DS), F32),
            pltpu.VMEM((8, 4, 2, 16, FA), BF16),
            pltpu.VMEM((8, 2, 4, 2, 8, FB), BF16),
            pltpu.VMEM((8, 2, 16, FA), BF16),
            pltpu.VMEM((8, 2, 2, 16, FA), BF16),
            pltpu.VMEM((8, 2, 8, FB), BF16),
            pltpu.VMEM((8, 2, 2, 8, FB), BF16),
            pltpu.VMEM((8, 4, 2, 8, FB), BF16),
            pltpu.VMEM((8, 16, FA), BF16),
            pltpu.VMEM((8, 16, FA), BF16),
            pltpu.VMEM((8, 4, 2, 16, FU), BF16),
            pltpu.VMEM((4, 8, 16, DS), BF16),
            pltpu.VMEM((4, 8, 16, DS), BF16),
            pltpu.VMEM((4, 8, 16, DS), BF16),
            pltpu.VMEM((8, 4, 16, DS), BF16),
            pltpu.VMEM((64, DS), BF16),
            pltpu.VMEM((64, 128), F32),
            pltpu.VMEM((8, 128), F32),
            pltpu.VMEM((8, 8, 128), F32),
            dma((4,)),
            dma((4,)),
            dma((2,)),
            dma((2,)),
            dma((2,)),
            dma((2,)),
            dma((16,)),
            dma((5,)),
            dma,
            dma((8, 3)),
            dma,
            dma((8, 3)),
            dma,
            dma((8, 3)),
            dma,
            dma((4,)),
            dma,
            dma,
            dma,
            dma,
        ],
        compiler_params=pltpu.CompilerParams(
            collective_id=0, has_side_effects=True, vmem_limit_bytes=56 * 1024 * 1024
        ),
        name="block",
    )(saved_input, keep_bits, norm_gain, gate_weight, up_weight, down_weight)
    return pl.pallas_call(
        finish,
        out_shape=(
            jax.ShapeDtypeStruct((64, DS), BF16),
            jax.ShapeDtypeStruct((64,), F32),
        ),
        in_specs=[hbm, hbm],
        out_specs=(hbm, hbm),
        scratch_shapes=[
            pltpu.VMEM((4, 16, DS), BF16),
            pltpu.VMEM((64,), F32),
            dma((2, 5)),
        ],
        name="finish",
    )(out, check)


def solution(mesh):
    both = ("dp", "tensor")
    return jax.shard_map(
        on_device,
        mesh=mesh,
        in_specs=(
            P(both, None),
            P(both, None),
            P("dp"),
            P("dp", "tensor"),
            P("dp", "tensor"),
            P("tensor", "dp"),
        ),
        out_specs=(P("tensor", "dp"), P("tensor")),
        check_vma=False,
    )
```
